256 devices in a mesh: dp: 16 (over y, x), expert: 16 (over z, core).
Axes of the slice: x: 4, y: 4, z: 8, core: 2. Of those that a mesh axis runs over, the one named last changes fastest.
Arguments:
- tokens: bfloat16 [4096, 4096], P('dp', 'expert'), may hold values from -6 to 6
- routing: int32 [4096, 2], P('dp'), may hold values from 0 to 15, all different within a row; in each aligned block of 256 rows (0 to 255, 256 to 511, ...) at most 48 rows name the same one
- gate_weight: bfloat16 [4096, 16], P('expert'), may hold values from -0.09375 to 0.09375
- expert_in: bfloat16 [16, 4096, 8192], P('dp', None, 'expert'), may hold values from -0.09375 to 0.09375
- expert_out: bfloat16 [16, 8192, 4096], P('dp', 'expert'), may hold values from -0.75 to 0.75
Outputs:
- mixed: bfloat16 [4096, 4096], P('dp', 'expert')
The draws below stay inside these ranges and needn't reach their ends.
Inputs may be any that keep to these rules, and one draw needn't show every extreme that they name: `routing`: each row names two different experts. Within the 256 rows of one group, no expert is named by more than 48 rows, a bound that some block reaches.
All inputs are finite; a program needn't handle non-finite values.
Results may differ from the reference program's by a relative error of at most 0.02.
Values may be sent and summed in bfloat16 or wider, within the bound.
A program may use at most 64 MiB of HBM per device.

```python
import math
import jax
import jax.numpy as jnp
import numpy as np
from jax import lax

D = 4096
FF = 8192
GROUP = 256
EXPERTS = 16
CAP = 48
TOKENS = 4096
N_DP = 16
N_EXPERT = 16


def strengthened(result, rng, source, target, blocks, factor):
    owner, partner = [(jnp.arange(result.shape[position]) // (result.shape[position] // blocks)).reshape([-1 if axis == position else 1 for axis in range(result.ndim)]) for position in (source, target)]
    chosen = jax.random.permutation(rng, blocks)[partner]
    strong = (owner == chosen) | (owner == (partner + blocks // 2) % blocks)
    return jnp.where(strong, factor * result, result)


def shard_levels(rng, shape, pieces, low, high):
    def one(position, blocks):
        heights = jax.random.uniform(jax.random.fold_in(jax.random.fold_in(rng, 6), position), (blocks,), jnp.float32, low / len(pieces), high / len(pieces))
        return jnp.repeat(jnp.exp(heights), shape[position] // blocks).reshape((-1,) + (1,) * (len(shape) - position - 1))

    factor_of = one(*pieces[0])
    for cut in pieces[1:]:
        factor_of = factor_of * one(*cut)
    return factor_of


def assign_block(stream_key, own, number, rows, count, top, bound, slope):
    sequence = jax.random.permutation(stream_key, count)
    crowded, ordinary = portions_of(count, rows * top, bound, slope, True), portions_of(count, rows * top, bound, slope, False)
    places = jnp.arange(count)

    def named(sizes, turn):
        used = int((sizes > 0).sum())
        fixed = max(1, used // 4)
        passed = fixed + (places - fixed + turn * (used - fixed)) % max(1, count - fixed)
        return jnp.zeros((count,), jnp.int32).at[sequence[jnp.where(places < fixed, places, passed)]].set(jnp.asarray(sizes, jnp.int32))

    sizes = jnp.where(number % 4 == 0, named(crowded, number // 4), named(ordinary, number - number // 4 - 1))
    mixed = jax.random.permutation(jax.random.fold_in(own, 3), count)
    donor, sink = mixed[0:count // 2 * 2:2], mixed[1:count // 2 * 2:2]
    room = jnp.minimum(sizes[donor] - 1, bound - sizes[sink]) // 2
    room = jnp.where((donor == sequence[0]) | (sink == sequence[0]) | (sizes[sink] == 0), 0, jnp.maximum(room, 0))
    passed = jax.random.randint(jax.random.fold_in(own, 4), (count // 2,), 0, 1 << 20) % (room + 1)
    sizes = sizes.at[donor].add(-passed).at[sink].add(passed)
    items = jnp.searchsorted(jnp.cumsum(sizes), jnp.arange(rows * top), side="right").astype(jnp.int32)
    table = items.reshape(top, rows).T
    table = table[jax.random.permutation(jax.random.fold_in(own, 1), rows)]
    turn = jax.random.randint(jax.random.fold_in(own, 2), (rows, 1), 0, top)
    return jnp.take_along_axis(table, (jnp.arange(top)[None, :] + turn) % top, axis=1)


def portions_of(count, total, most, slope, full):
    weights = [(1 << 20) // math.isqrt(grade ** slope) + 1 for grade in range(1, count + 1)]
    largest = most if full else min(most, max(-(-total // count), total * weights[0] // sum(weights)))
    least = 1 if total - largest >= count - 1 else 0
    counts, surplus = [largest] + [least] * (count - 1), total - largest - least * (count - 1)
    while surplus > 0:
        candidates = [i for i in range(1, count) if counts[i] < largest] or [i for i in range(1, count) if counts[i] < most]
        whole, left = sum([weights[i] for i in candidates]), surplus
        for i in candidates:
            more = min(most - counts[i], max(1, left * weights[i] // whole), surplus)
            counts[i] = counts[i] + more
            surplus = surplus - more
    return np.array(counts)


def centred(rng, dims, deviation, most, shards=(), kind=jnp.bfloat16):
    result = deviation * jax.random.normal(rng, dims, jnp.float32)
    if shards:
        result = result * shard_levels(rng, dims, shards, -0.22, 0.18)
    return jnp.clip(result, -most, most).astype(kind)


def noise_with(key, shape, deviation, bound, shards, heavy, kind=jnp.bfloat16):
    array = deviation * jax.random.normal(key, shape, jnp.float32)
    if shards:
        array = array * shard_levels(key, shape, shards, -0.22, 0.18)
    return jnp.clip(strengthened(array, jax.random.fold_in(key, 3), *heavy), -bound, bound).astype(kind)


def setup_inputs(seed: int = 0) -> dict:
    streams_of = jax.random.split(jax.random.key(seed), 6)
    tokens = centred(streams_of[0], (TOKENS, D), 1.0, 6.0, ((0, 16), (1, 16)))
    routing_keys = jax.random.split(jax.random.fold_in(streams_of[1], 1), TOKENS // GROUP)
    routing_turns = jax.random.permutation(jax.random.fold_in(streams_of[1], 3), TOKENS // GROUP)
    routing = jax.vmap(lambda own, number: assign_block(jax.random.fold_in(streams_of[1], 2), own, number, GROUP, EXPERTS, 2, CAP, 2))(routing_keys, routing_turns).reshape((TOKENS, 2))
    gate_weight = centred(streams_of[2], (D, EXPERTS), D ** -0.5, 0.09375, ((0, 16),))
    expert_in = centred(streams_of[3], (EXPERTS, D, FF), D ** -0.5, 0.09375, ((0, 16), (2, 16)))
    expert_out = noise_with(streams_of[4], (EXPERTS, FF, D), (FF // 64) ** -0.5, 0.75, ((0, 16), (1, 16)), (1, 2, 16, 2.0))
    return {"tokens": tokens, "routing": routing, "gate_weight": gate_weight, "expert_in": expert_in, "expert_out": expert_out}


def slot_table(grouped):
    order = jnp.transpose(grouped, (0, 2, 1)).reshape(grouped.shape[0], -1)
    onehot = (order[:, :, None] == jnp.arange(EXPERTS, dtype=jnp.int32)[None, None, :]).astype(jnp.int32)
    before = jnp.cumsum(onehot, axis=1) - onehot
    slot_flat = jnp.sum(before * onehot, axis=-1).astype(jnp.int32)
    return jnp.transpose(slot_flat.reshape(grouped.shape[0], 2, -1), (0, 2, 1))


def reference(tokens, routing, gate_weight, expert_in, expert_out):
    logits = jnp.dot(tokens, gate_weight, preferred_element_type=jnp.float32)
    raised = jnp.exp(logits)
    softmax_all = raised / jnp.sum(raised, axis=-1, keepdims=True)
    chosen = jnp.take_along_axis(softmax_all, routing, axis=1).astype(jnp.bfloat16)
    grouped = routing.reshape(N_DP, GROUP, 2)
    slot_index = slot_table(grouped)
    group_ids = jnp.broadcast_to(jnp.arange(N_DP, dtype=jnp.int32)[:, None, None], (N_DP, GROUP, 2))
    token_rows = jnp.broadcast_to(tokens.reshape(N_DP, GROUP, 1, D), (N_DP, GROUP, 2, D))
    buffer = jnp.zeros((EXPERTS, N_DP, CAP, D), jnp.bfloat16)
    buffer = buffer.at[grouped, group_ids, slot_index].set(token_rows)
    width_block = FF // N_EXPERT

    def run_expert(packed):
        rows_in, weight_in, weight_out = packed
        flat_rows = rows_in.reshape(N_DP * CAP, D)
        hidden = jax.nn.gelu(jnp.dot(flat_rows, weight_in, preferred_element_type=jnp.float32), approximate=True).astype(jnp.bfloat16)

        def add_block(index, running):
            start = (index * width_block).astype(jnp.int32)
            left = lax.dynamic_slice_in_dim(hidden, start, width_block, 1)
            right = lax.dynamic_slice_in_dim(weight_out, start, width_block, 0)
            term = jnp.dot(left, right, preferred_element_type=jnp.float32).astype(jnp.bfloat16)
            term = lax.optimization_barrier(term)
            return running + term.astype(jnp.float32)

        summed = lax.fori_loop(0, N_EXPERT, add_block, jnp.zeros((N_DP * CAP, D), jnp.float32))
        return summed.astype(jnp.bfloat16).reshape(N_DP, CAP, D)

    expert_result = lax.map(run_expert, (buffer, expert_in, expert_out))
    picked = expert_result[grouped, group_ids, slot_index]
    weights = chosen.reshape(N_DP, GROUP, 2, 1).astype(jnp.float32)
    mixed = jnp.sum(picked.astype(jnp.float32) * weights, axis=2)
    return mixed.reshape(TOKENS, D).astype(jnp.bfloat16)
```

```python
import functools

import jax
import jax.numpy as jnp
from jax import lax
from jax.experimental import pallas as pl
from jax.experimental.pallas import tpu as pltpu
from jax.sharding import PartitionSpec as P

MESH = pl.DeviceIdType.MESH
F32 = jnp.float32
BF16 = jnp.bfloat16

X, Y, Z = 4, 4, 8
GROUP, CAP, EXPERTS, W, HID = 256, 48, 16, 256, 512
SHIFTS = [(dx, dy) for dy in (-1, 0, 1) for dx in (-1, 0, 1)]
SHIFTS += [(2, dy) for dy in (-1, 0, 1, 2)] + [(dx, 2) for dx in (-1, 0, 1)]
NEAR, FAR, SELF = 9, 7, 4
NR, FR = NEAR * CAP, FAR * CAP
NEAR_ORDER = [1, 3, 7, 5, 0, 8, 2, 6]
FAR_ORDER = [12, 9, 11, 13, 15, 10, 14]
TB = GROUP + EXPERTS
T_HALF = ((0, 128), (128, TB - 128))
F_HALF = ((0, 192), (192, FR - 192))
M_HALF = ((0, 128), (128, 128))


def parts_of(step):
    return ((0, 0), (1, 1)) if step == 4 else ((0, 0), (1, 1), (0, 1), (1, 0))


def back_parts_of(step):
    return ((0, 0), (1, 1)) if step == 1 else ((0, 0), (1, 1), (0, 1), (1, 0))


def offset_of(slot):
    return 4 if slot == 7 else (slot // 2 if slot % 2 == 0 else -((slot + 1) // 2))


def gather_slots(step, way):
    source = 0 if step == 1 else 2 * step - 3 + way
    return source, (7 if step == 4 else 2 * step - 1 + way)


def back_slot(step, way):
    return 7 if step == 1 else 2 * (5 - step) - way


def kernel(
    tokens, routing, gate, w_in, w_out, out,
    tg, assign, near_send, far_send, xn, xf, acc_n, acc_f, w1, w2, hn, hf,
    pf, rf, pn, rn, pm, rm, fr, ra, cn, cf, lg, lg_other, base,
    tok_sem, w1_sem, w2_sem, w2s_send, w2s_recv,
    f1_send, f1_recv, a1_send, a1_recv, f2_send, f2_recv, a2_send, a2_recv,
    sn_send, sn_recv, sf_send, sf_recv, h_send, h_recv, l_send, l_recv,
    bf_send, bf_recv, bn_send, bn_recv, bm_send, bm_recv, ra_send, ra_recv,
):
    dp = lax.axis_index("dp")
    ex = lax.axis_index("expert")
    gy, gx = lax.div(dp, X), lax.rem(dp, X)
    z, core = lax.div(ex, 2), lax.rem(ex, 2)

    def plane(dx, dy):
        return (lax.rem(gy + dy + Y, Y) * X + lax.rem(gx + dx + X, X), ex)

    def ring(offset):
        return lax.rem(z + offset + Z, Z)

    to = [plane(dx, dy) for dx, dy in SHIFTS]
    back = [plane(-dx, -dy) for dx, dy in SHIFTS]
    along = ((dp, ring(1) * 2 + core), (dp, ring(-1) * 2 + core))
    sibling = (dp, z * 2 + 1 - core)

    def remote(src, dst, send, recv, device):
        return pltpu.make_async_remote_copy(
            src_ref=src, dst_ref=dst, send_sem=send, recv_sem=recv,
            device_id=device, device_id_type=MESH,
        )

    barrier = pltpu.get_barrier_semaphore()
    for device in [to[p] for p in range(EXPERTS) if p != SELF] + [*along, sibling]:
        pl.semaphore_signal(barrier, inc=1, device_id=device, device_id_type=MESH)

    token_copy = pltpu.make_async_copy(tokens, tg.at[0, pl.ds(0, GROUP)], tok_sem)
    token_copy.start()
    tg[0, GROUP:TB, :] = gate[...]

    def w1_copy(slot, side):
        rows = (ring(offset_of(slot)) * 2 + (core if side == 0 else 1 - core)) * W
        return pltpu.make_async_copy(
            w_in.at[0, pl.ds(pl.multiple_of(rows, W), W), :], w1.at[slot, side], w1_sem.at[slot, side]
        )

    def w2_columns(slot, side):
        columns = (ring(offset_of(slot)) * 2 + (core if side == 0 else 1 - core)) * W
        return w_out.at[0, :, pl.ds(pl.multiple_of(columns, W), W)]

    def w2_copy(slot):
        return pltpu.make_async_copy(w2_columns(slot, 0), w2.at[slot, pl.ds(0, HID)], w2_sem.at[slot])

    def w2_share(slot):
        return remote(
            w2_columns(slot, 1), w2.at[slot, pl.ds(HID, HID)], w2s_send.at[slot], w2s_recv.at[slot], sibling
        )

    for slot in range(Z):
        for side in range(2):
            w1_copy(slot, side).start()
    for slot in range(Z):
        w2_copy(slot).start()

    names = lax.broadcasted_iota(jnp.int32, (EXPERTS, GROUP), 0)
    sx = (lax.rem(names, X) - gx + 1 + X) & 3
    sy = (lax.div(names, X) - gy + 1 + Y) & 3
    place = jnp.where(sx == 3, NEAR + sy, jnp.where(sy == 3, 13 + sx, sy * 3 + sx))
    place = (place * CAP).astype(F32)
    first = (names == routing[0:1, :]).astype(F32)
    second = (names == routing[1:2, :]).astype(F32)
    earlier = lax.broadcasted_iota(jnp.int32, (GROUP, GROUP), 0)
    later = lax.broadcasted_iota(jnp.int32, (GROUP, GROUP), 1)
    upper = (earlier < later).astype(F32).astype(BF16)
    before_first = jnp.dot(first.astype(BF16), upper, preferred_element_type=F32)
    before_second = jnp.dot(second.astype(BF16), upper, preferred_element_type=F32)
    before_second = before_second + jnp.sum(first, axis=1, keepdims=True)
    row_first = jnp.sum(first * (place + before_first), axis=0, keepdims=True)
    row_second = jnp.sum(second * (place + before_second), axis=0, keepdims=True)
    rows = lax.broadcasted_iota(jnp.int32, (EXPERTS * CAP, GROUP), 0)
    hit = (rows == row_first.astype(jnp.int32)) | (rows == row_second.astype(jnp.int32))
    assign[...] = hit.astype(F32).astype(BF16)
    base[0:1, :] = row_first
    base[1:2, :] = row_second
    lg[...] = jnp.zeros_like(lg)

    token_copy.wait()
    far_send[...] = jnp.dot(
        assign[NR:, :], tg[0, 0:GROUP, :], preferred_element_type=F32
    ).astype(BF16)

    def dispatch_near(slot):
        rows_of = jnp.dot(assign[0:NR, :], tg[slot, 0:GROUP, :], preferred_element_type=F32).astype(BF16)
        near_send[slot] = rows_of
        xn[slot, 0, SELF * CAP:(SELF + 1) * CAP, :] = rows_of[SELF * CAP:(SELF + 1) * CAP, :]
        lg[...] += lax.dot_general(
            tg[slot, GROUP:TB, :], tg[slot, 0:GROUP, :], (((1,), (1,)), ((), ())), preferred_element_type=F32
        )

    dispatch_near(0)

    pl.semaphore_wait(barrier, 18)

    def f1(step, way, half):
        source, target = gather_slots(step, way)
        start, size = T_HALF[half]
        return remote(
            tg.at[source, pl.ds(start, size)], tg.at[target, pl.ds(start, size)],
            f1_send.at[step - 1, way, half], f1_recv.at[step - 1, way, half], along[way],
        )

    def a1(p):
        block = pl.ds((p - NEAR) * CAP, CAP)
        return remote(far_send.at[block], xf.at[0, 0, block], a1_send, a1_recv, to[p])

    def f2(slot, p):
        block = pl.ds(p * CAP, CAP)
        return remote(
            near_send.at[slot, block], xn.at[slot, 0, block], f2_send.at[slot], f2_recv.at[slot], to[p]
        )

    def f2_all(slot):
        block = pl.ds(0, NR - CAP)
        return remote(
            near_send.at[slot, block], xn.at[slot, 0, block], f2_send.at[slot], f2_recv.at[slot], sibling
        )

    def a2(step, way, half):
        source, target = gather_slots(step, way)
        start, size = F_HALF[half]
        return remote(
            xf.at[source, 0, pl.ds(start, size)], xf.at[target, 0, pl.ds(start, size)],
            a2_send.at[step - 1, way, half], a2_recv.at[step - 1, way, half], along[way],
        )

    def share_near(slot):
        return remote(xn.at[slot, 0], xn.at[slot, 1], sn_send.at[slot], sn_recv.at[slot], sibling)

    def share_far(slot):
        return remote(xf.at[slot, 0], xf.at[slot, 1], sf_send.at[slot], sf_recv.at[slot], sibling)

    def send_near(slot):
        for p in NEAR_ORDER:
            f2(slot, p).start()

    def pass_on(transfer, step):
        for way, half in parts_of(step):
            transfer(step, way, half).wait_recv()
            if step < 4 and (way, half) in parts_of(step + 1):
                transfer(step + 1, way, half).start()

    for way, half in parts_of(1):
        f1(1, way, half).start()
    for p in FAR_ORDER:
        a1(p).start()
    send_near(0)

    acc_n[...] = jnp.zeros_like(acc_n)
    acc_f[...] = jnp.zeros_like(acc_f)

    def both(lower, upper, work):
        lax.fori_loop(lower, upper, lambda slot, carry: (work(slot), carry)[1], 0)

    def near_part(slot):
        dispatch_near(slot)
        send_near(slot)

    def multiply(rows_of, total, side):
        def work(slot):
            total[...] += jnp.dot(rows_of[slot, side], w1[slot, side], preferred_element_type=F32)

        return work

    def near_in(slot):
        f2_all(slot).wait_recv()
        share_near(slot).start()

    def near_multiply(slot):
        multiply(xn, acc_n, 0)(slot)
        share_near(slot).wait_recv()
        multiply(xn, acc_n, 1)(slot)

    def far_multiply(slot):
        multiply(xf, acc_f, 0)(slot)
        share_far(slot).wait_recv()
        multiply(xf, acc_f, 1)(slot)

    pass_on(f1, 1)
    both(1, 3, near_part)
    pl_all = pl.ds(0, FR)
    remote(far_send.at[pl_all], xf.at[0, 0, pl_all], a1_send, a1_recv, sibling).wait_recv()
    for way, half in parts_of(1):
        a2(1, way, half).start()
    share_far(0).start()
    pass_on(f1, 2)
    both(3, 5, near_part)
    near_in(0)
    pass_on(a2, 1)
    share_far(1).start()
    share_far(2).start()
    pass_on(f1, 3)
    both(5, 7, near_part)
    for slot in range(Z):
        w2_share(slot).start()
    for slot in range(Z):
        for side in range(2):
            w1_copy(slot, side).wait()
    both(1, 3, near_in)
    pass_on(f1, 4)
    both(7, 8, near_part)

    logit_copy = remote(lg, lg_other, l_send, l_recv, sibling)
    logit_copy.start()
    pass_on(a2, 2)
    share_far(3).start()
    share_far(4).start()

    def first_multiplies(slot):
        near_multiply(slot)
        far_multiply(slot)

    both(0, 3, first_multiplies)
    both(3, 7, near_in)
    pass_on(a2, 3)
    share_far(5).start()
    share_far(6).start()
    both(3, 7, near_multiply)
    near_in(7)

    logit_copy.wait()
    raised = jnp.exp(lg[...] + lg_other[...])
    probs = raised / jnp.sum(raised, axis=0, keepdims=True)
    chosen_first = jnp.sum(jnp.where(names == routing[0:1, :], probs, 0.0), axis=0, keepdims=True)
    chosen_second = jnp.sum(jnp.where(names == routing[1:2, :], probs, 0.0), axis=0, keepdims=True)
    packed = jnp.concatenate(
        [base[0:1, :], base[1:2, :], chosen_first, chosen_second, jnp.zeros((124, GROUP), F32)], axis=0
    )
    packed = jnp.transpose(packed)
    at_first, at_second = packed[:, 0:1].astype(jnp.int32), packed[:, 1:2].astype(jnp.int32)
    by_first, by_second = packed[:, 2:3], packed[:, 3:4]

    def weights(start, size):
        columns = lax.broadcasted_iota(jnp.int32, (GROUP, size), 1) + start
        return (
            jnp.where(columns == at_first, by_first, 0.0) + jnp.where(columns == at_second, by_second, 0.0)
        ).astype(BF16)

    cn[...] = weights(0, NR)
    cf[...] = weights(NR, FR)

    both(7, 8, near_multiply)

    def share_hidden(buffer, which):
        return remote(
            buffer.at[0], buffer.at[1], h_send.at[which], h_recv.at[which], sibling
        )

    hn[0] = jax.nn.gelu(acc_n[...], approximate=True).astype(BF16)
    share_hidden(hn, 0).start()
    pass_on(a2, 4)
    share_far(7).start()
    both(3, 7, far_multiply)
    for slot in range(Z):
        w2_copy(slot).wait()
        w2_share(slot).wait_recv()

    def bn(slot, p):
        block = pl.ds(p * CAP, CAP)
        return remote(
            pn.at[slot, block], rn.at[slot, block], bn_send.at[slot], bn_recv.at[slot], back[p]
        )

    def bn_all(slot):
        block = pl.ds(0, NR - CAP)
        return remote(
            pn.at[slot, block], rn.at[slot, block], bn_send.at[slot], bn_recv.at[slot], sibling
        )

    def second(buffer, slot):
        return (
            jnp.dot(buffer[0], w2[slot, 0:HID, :], preferred_element_type=F32)
            + jnp.dot(buffer[1], w2[slot, HID:2 * HID, :], preferred_element_type=F32)
        ).astype(BF16)

    def near_out(index):
        slot = 7 - index
        terms = second(hn, slot)
        pn[slot] = terms
        rn[slot, SELF * CAP:(SELF + 1) * CAP, :] = terms[SELF * CAP:(SELF + 1) * CAP, :]
        for p in NEAR_ORDER:
            bn(slot, p).start()

    share_hidden(hn, 0).wait_recv()
    both(0, 4, near_out)
    both(7, 8, far_multiply)
    hf[0] = jax.nn.gelu(acc_f[...], approximate=True).astype(BF16)
    share_hidden(hf, 1).start()
    both(4, 8, near_out)
    share_hidden(hf, 1).wait_recv()

    def far_out(index):
        slot = 7 - index
        pf[slot] = second(hf, slot)

    def reduce_copy(own, received, halves, send, recv, step, way, half):
        start, size = halves[half]
        return remote(
            own.at[back_slot(step, way), pl.ds(start, size)], received.at[way, step - 1, pl.ds(start, size)],
            send.at[step - 1, way, half], recv.at[step - 1, way, half], along[way],
        )

    bf = functools.partial(reduce_copy, pf, rf, F_HALF, bf_send, bf_recv)
    bm = functools.partial(reduce_copy, pm, rm, M_HALF, bm_send, bm_recv)

    def reduce_step(transfer, own, received, halves, step):
        for way, half in back_parts_of(step):
            if step > 1 and (way, half) in back_parts_of(step - 1):
                transfer(step - 1, way, half).wait_recv()
                start, size = halves[half]
                slot = back_slot(step, way)
                own[slot, start:start + size, :] = (
                    own[slot, start:start + size, :].astype(F32)
                    + received[way, step - 2, start:start + size, :].astype(F32)
                ).astype(BF16)
            transfer(step, way, half).start()

    def mix(slot):
        bn_all(slot).wait_recv()
        pm[slot] = jnp.dot(cn[...], rn[slot], preferred_element_type=F32).astype(BF16)

    def mix_down(index):
        mix(7 - index)

    both(0, 1, far_out)
    reduce_step(bf, pf, rf, F_HALF, 1)
    both(1, 3, far_out)
    both(0, 1, mix_down)
    reduce_step(bm, pm, rm, M_HALF, 1)
    both(3, 8, far_out)
    reduce_step(bf, pf, rf, F_HALF, 2)
    both(1, 3, mix_down)
    reduce_step(bm, pm, rm, M_HALF, 2)
    both(3, 5, mix_down)
    reduce_step(bf, pf, rf, F_HALF, 3)
    reduce_step(bm, pm, rm, M_HALF, 3)
    both(5, 8, mix_down)
    reduce_step(bf, pf, rf, F_HALF, 4)
    reduce_step(bm, pm, rm, M_HALF, 4)

    for way, half in back_parts_of(4):
        bf(4, way, half).wait_recv()
    fr[...] = (
        pf[0].astype(F32) + rf[0, 3].astype(F32) + rf[1, 3].astype(F32)
    ).astype(BF16)

    def far_back(p):
        block = pl.ds((p - NEAR) * CAP, CAP)
        return remote(fr.at[block], ra.at[block], ra_send, ra_recv, back[p])

    for p in FAR_ORDER:
        far_back(p).start()
    for way, half in back_parts_of(4):
        bm(4, way, half).wait_recv()
    partial = pm[0].astype(F32) + rm[0, 3].astype(F32) + rm[1, 3].astype(F32)
    remote(fr, ra, ra_send, ra_recv, sibling).wait_recv()
    out[...] = (partial + jnp.dot(cf[...], ra[...], preferred_element_type=F32)).astype(BF16)

    for step in range(1, 5):
        for way, half in parts_of(step):
            f1(step, way, half).wait_send()
            a2(step, way, half).wait_send()
        for way, half in back_parts_of(step):
            bf(step, way, half).wait_send()
            bm(step, way, half).wait_send()
    remote(far_send.at[pl_all], xf.at[0, 0, pl_all], a1_send, a1_recv, sibling).wait_send()
    remote(fr, ra, ra_send, ra_recv, sibling).wait_send()

    def sent(slot):
        f2_all(slot).wait_send()
        bn_all(slot).wait_send()
        share_near(slot).wait_send()
        share_far(slot).wait_send()

    both(0, Z, sent)
    for slot in range(Z):
        w2_share(slot).wait_send()
    share_hidden(hn, 0).wait_send()
    share_hidden(hf, 1).wait_send()


def layer(tokens, routing, gate_weight, expert_in, expert_out):
    vmem = pl.BlockSpec(memory_space=pltpu.VMEM)
    anywhere = pl.BlockSpec(memory_space=pl.ANY)
    dma = pltpu.SemaphoreType.DMA
    return pl.pallas_call(
        kernel,
        out_shape=jax.ShapeDtypeStruct((GROUP, W), BF16),
        in_specs=[anywhere, vmem, vmem, anywhere, anywhere],
        out_specs=vmem,
        scratch_shapes=[
            pltpu.VMEM((Z, TB, W), BF16),
            pltpu.VMEM((EXPERTS * CAP, GROUP), BF16),
            pltpu.VMEM((Z, NR, W), BF16),
            pltpu.VMEM((FR, W), BF16),
            pltpu.VMEM((Z, 2, NR, W), BF16),
            pltpu.VMEM((Z, 2, FR, W), BF16),
            pltpu.VMEM((NR, HID), F32),
            pltpu.VMEM((FR, HID), F32),
            pltpu.VMEM((Z, 2, W, HID), BF16),
            pltpu.VMEM((Z, 2 * HID, W), BF16),
            pltpu.VMEM((2, NR, HID), BF16),
            pltpu.VMEM((2, FR, HID), BF16),
            pltpu.VMEM((Z, FR, W), BF16),
            pltpu.VMEM((2, 4, FR, W), BF16),
            pltpu.VMEM((Z, NR, W), BF16),
            pltpu.VMEM((Z, NR, W), BF16),
            pltpu.VMEM((Z, GROUP, W), BF16),
            pltpu.VMEM((2, 4, GROUP, W), BF16),
            pltpu.VMEM((FR, W), BF16),
            pltpu.VMEM((FR, W), BF16),
            pltpu.VMEM((GROUP, NR), BF16),
            pltpu.VMEM((GROUP, FR), BF16),
            pltpu.VMEM((EXPERTS, GROUP), F32),
            pltpu.VMEM((EXPERTS, GROUP), F32),
            pltpu.VMEM((8, GROUP), F32),
            dma, dma((Z, 2)), dma((Z,)), dma((Z,)), dma((Z,)),
            dma((4, 2, 2)), dma((4, 2, 2)), dma, dma, dma((Z,)), dma((Z,)), dma((4, 2, 2)), dma((4, 2, 2)),
            dma((Z,)), dma((Z,)), dma((Z,)), dma((Z,)), dma((2,)), dma((2,)), dma, dma,
            dma((4, 2, 2)), dma((4, 2, 2)), dma((Z,)), dma((Z,)), dma((4, 2, 2)), dma((4, 2, 2)), dma, dma,
        ],
        compiler_params=pltpu.CompilerParams(collective_id=0, has_side_effects=True),
        name="experts",
    )(tokens, routing.T, gate_weight.T, expert_in, expert_out)


def solution(mesh):
    return jax.shard_map(
        layer,
        mesh=mesh,
        in_specs=(
            P("dp", "expert"),
            P("dp", None),
            P("expert", None),
            P("dp", None, "expert"),
            P("dp", "expert", None),
        ),
        out_specs=P("dp", "expert"),
        check_vma=False,
    )
```

```python
import functools

import jax
import jax.numpy as jnp
from jax import lax
from jax.experimental import pallas as pl
from jax.experimental.pallas import tpu as pltpu
from jax.sharding import PartitionSpec as P

MESH = pl.DeviceIdType.MESH
F32 = jnp.float32
BF16 = jnp.bfloat16

X, Y, Z = 4, 4, 8
GROUP, CAP, EXPERTS, W, HID = 256, 48, 16, 256, 512
SHIFTS = [(dx, dy) for dy in (-1, 0, 1) for dx in (-1, 0, 1)]
SHIFTS += [(2, 0), (0, 2), (2, -1), (2, 1), (2, 2), (-1, 2), (1, 2)]
NEAR, FAR, SELF = 11, 5, 4
NR, FR = NEAR * CAP, FAR * CAP
NEAR_ORDER = [1, 3, 7, 5, 9, 10, 0, 8, 2, 6]
FAR_ORDER = [13, 11, 14, 12, 15]
TB = GROUP + EXPERTS
T_HALF = ((0, 128), (128, TB - 128))
F_HALF = ((0, 3 * CAP), (3 * CAP, FR - 3 * CAP))
M_HALF = ((0, 128), (128, 128))


def parts_of(step):
    return ((0, 0), (1, 1)) if step == 4 else ((0, 0), (1, 1), (0, 1), (1, 0))


def back_parts_of(step):
    return ((0, 0), (1, 1)) if step == 1 else ((0, 0), (1, 1), (0, 1), (1, 0))


def offset_of(slot):
    return 4 if slot == 7 else (slot // 2 if slot % 2 == 0 else -((slot + 1) // 2))


def gather_slots(step, way):
    source = 0 if step == 1 else 2 * step - 3 + way
    return source, (7 if step == 4 else 2 * step - 1 + way)


def back_slot(step, way):
    return 7 if step == 1 else 2 * (5 - step) - way


def kernel(
    tokens, routing, gate, w_in, w_out, out,
    tg, assign, near_send, far_send, xn, xf, acc_n, acc_f, w1, w2, hn, hf,
    pf, rf, pn, rn, pm, rm, fr, ra, cn, cf, lg, lg_other, base, far_term,
    tok_sem, w1_sem, w2_sem, w2s_send, w2s_recv,
    f1_send, f1_recv, a1_send, a1_recv, f2_send, f2_recv, a2_send, a2_recv,
    sn_send, sn_recv, sf_send, sf_recv, h_send, h_recv, l_send, l_recv,
    bf_send, bf_recv, bn_send, bn_recv, bm_send, bm_recv, ra_send, ra_recv,
):
    dp = lax.axis_index("dp")
    ex = lax.axis_index("expert")
    gy, gx = lax.div(dp, X), lax.rem(dp, X)
    z, core = lax.div(ex, 2), lax.rem(ex, 2)

    def plane(dx, dy):
        return (lax.rem(gy + dy + Y, Y) * X + lax.rem(gx + dx + X, X), ex)

    def ring(offset):
        return lax.rem(z + offset + Z, Z)

    to = [plane(dx, dy) for dx, dy in SHIFTS]
    back = [plane(-dx, -dy) for dx, dy in SHIFTS]
    along = ((dp, ring(1) * 2 + core), (dp, ring(-1) * 2 + core))
    sibling = (dp, z * 2 + 1 - core)

    def remote(src, dst, send, recv, device):
        return pltpu.make_async_remote_copy(
            src_ref=src, dst_ref=dst, send_sem=send, recv_sem=recv,
            device_id=device, device_id_type=MESH,
        )

    barrier = pltpu.get_barrier_semaphore()
    for device in [to[p] for p in range(EXPERTS) if p != SELF] + [*along, sibling]:
        pl.semaphore_signal(barrier, inc=1, device_id=device, device_id_type=MESH)

    token_copy = pltpu.make_async_copy(tokens, tg.at[0, pl.ds(0, GROUP)], tok_sem)
    token_copy.start()
    tg[0, GROUP:TB, :] = gate[...]

    def w1_copy(slot, side):
        rows = (ring(offset_of(slot)) * 2 + (core if side == 0 else 1 - core)) * W
        return pltpu.make_async_copy(
            w_in.at[0, pl.ds(pl.multiple_of(rows, W), W), :], w1.at[slot, side], w1_sem.at[slot, side]
        )

    def w2_columns(slot, side):
        columns = (ring(offset_of(slot)) * 2 + (core if side == 0 else 1 - core)) * W
        return w_out.at[0, :, pl.ds(pl.multiple_of(columns, W), W)]

    def w2_copy(slot):
        return pltpu.make_async_copy(w2_columns(slot, 0), w2.at[slot, pl.ds(0, HID)], w2_sem.at[slot])

    def w2_share(slot):
        return remote(
            w2_columns(slot, 1), w2.at[slot, pl.ds(HID, HID)], w2s_send.at[slot], w2s_recv.at[slot], sibling
        )

    def f1(step, way, half):
        source, target = gather_slots(step, way)
        start, size = T_HALF[half]
        return remote(
            tg.at[source, pl.ds(start, size)], tg.at[target, pl.ds(start, size)],
            f1_send.at[step - 1, way, half], f1_recv.at[step - 1, way, half], along[way],
        )

    def a1(p):
        block = pl.ds((p - NEAR) * CAP, CAP)
        return remote(far_send.at[block], xf.at[0, 0, block], a1_send, a1_recv, to[p])

    def f2(slot, p):
        block = pl.ds(p * CAP, CAP)
        return remote(
            near_send.at[slot, block], xn.at[slot, 0, block], f2_send.at[slot], f2_recv.at[slot], to[p]
        )

    def f2_all(slot):
        block = pl.ds(0, NR - CAP)
        return remote(
            near_send.at[slot, block], xn.at[slot, 0, block], f2_send.at[slot], f2_recv.at[slot], sibling
        )

    def a2(step, way, half):
        source, target = gather_slots(step, way)
        start, size = F_HALF[half]
        return remote(
            xf.at[source, 0, pl.ds(start, size)], xf.at[target, 0, pl.ds(start, size)],
            a2_send.at[step - 1, way, half], a2_recv.at[step - 1, way, half], along[way],
        )

    def share_near(slot):
        return remote(xn.at[slot, 0], xn.at[slot, 1], sn_send.at[slot], sn_recv.at[slot], sibling)

    def share_far(slot):
        return remote(xf.at[slot, 0], xf.at[slot, 1], sf_send.at[slot], sf_recv.at[slot], sibling)

    def send_near(slot):
        for p in NEAR_ORDER:
            f2(slot, p).start()

    def pass_on(transfer, step):
        for way, half in parts_of(step):
            transfer(step, way, half).wait_recv()
            if step < 4 and (way, half) in parts_of(step + 1):
                transfer(step + 1, way, half).start()

    names = lax.broadcasted_iota(jnp.int32, (EXPERTS, GROUP), 0)
    sx = (lax.rem(names, X) - gx + 1 + X) & 3
    sy = (lax.div(names, X) - gy + 1 + Y) & 3
    place = sy * 3 + sx
    for p in range(9, EXPERTS):
        dx, dy = SHIFTS[p]
        place = jnp.where((sx == dx + 1) & (sy == dy + 1), p, place)
    place = (place * CAP).astype(F32)
    first = (names == routing[0:1, :]).astype(F32)
    second = (names == routing[1:2, :]).astype(F32)
    earlier = lax.broadcasted_iota(jnp.int32, (GROUP, GROUP), 0)
    later = lax.broadcasted_iota(jnp.int32, (GROUP, GROUP), 1)
    upper = (earlier < later).astype(F32).astype(BF16)
    before_first = jnp.dot(first.astype(BF16), upper, preferred_element_type=F32)
    before_second = jnp.dot(second.astype(BF16), upper, preferred_element_type=F32)
    before_second = before_second + jnp.sum(first, axis=1, keepdims=True)
    row_first = jnp.sum(first * (place + before_first), axis=0, keepdims=True)
    row_second = jnp.sum(second * (place + before_second), axis=0, keepdims=True)
    rows = lax.broadcasted_iota(jnp.int32, (EXPERTS * CAP, GROUP), 0)
    hit = (rows == row_first.astype(jnp.int32)) | (rows == row_second.astype(jnp.int32))
    assign[...] = hit.astype(F32).astype(BF16)
    base[0:1, :] = row_first
    base[1:2, :] = row_second
    lg[...] = jnp.zeros_like(lg)

    token_copy.wait()
    pl.semaphore_wait(barrier, 18)
    for way, half in parts_of(1):
        f1(1, way, half).start()
    far_send[...] = jnp.dot(
        assign[NR:, :], tg[0, 0:GROUP, :], preferred_element_type=F32
    ).astype(BF16)

    def dispatch_near(slot):
        rows_of = jnp.dot(assign[0:NR, :], tg[slot, 0:GROUP, :], preferred_element_type=F32).astype(BF16)
        near_send[slot] = rows_of
        xn[slot, 0, SELF * CAP:(SELF + 1) * CAP, :] = rows_of[SELF * CAP:(SELF + 1) * CAP, :]
        lg[...] += lax.dot_general(
            tg[slot, GROUP:TB, :], tg[slot, 0:GROUP, :], (((1,), (1,)), ((), ())), preferred_element_type=F32
        )

    for p in FAR_ORDER:
        a1(p).start()
    dispatch_near(0)
    send_near(0)
    for slot in range(Z):
        for side in range(2):
            w1_copy(slot, side).start()
    for slot in range(Z):
        w2_copy(slot).start()

    acc_n[...] = jnp.zeros_like(acc_n)
    acc_f[...] = jnp.zeros_like(acc_f)

    def both(lower, upper, work):
        lax.fori_loop(lower, upper, lambda slot, carry: (work(slot), carry)[1], 0)

    def near_part(slot):
        dispatch_near(slot)
        send_near(slot)

    def multiply(rows_of, total, side):
        def work(slot):
            total[...] += jnp.dot(rows_of[slot, side], w1[slot, side], preferred_element_type=F32)

        return work

    def near_in(slot):
        f2_all(slot).wait_recv()
        share_near(slot).start()

    def near_multiply(slot):
        multiply(xn, acc_n, 0)(slot)
        share_near(slot).wait_recv()
        multiply(xn, acc_n, 1)(slot)

    def far_multiply(slot):
        multiply(xf, acc_f, 0)(slot)
        share_far(slot).wait_recv()
        multiply(xf, acc_f, 1)(slot)

    pass_on(f1, 1)
    both(1, 3, near_part)
    pl_all = pl.ds(0, FR)
    remote(far_send.at[pl_all], xf.at[0, 0, pl_all], a1_send, a1_recv, sibling).wait_recv()
    for way, half in parts_of(1):
        a2(1, way, half).start()
    share_far(0).start()
    pass_on(f1, 2)
    both(3, 5, near_part)
    near_in(0)
    for slot in range(Z):
        for side in range(2):
            w1_copy(slot, side).wait()
    both(0, 1, far_multiply)
    pass_on(a2, 1)
    share_far(1).start()
    share_far(2).start()
    both(0, 1, near_multiply)
    pass_on(f1, 3)
    both(5, 7, near_part)
    both(1, 3, near_in)
    for slot in range(Z):
        w2_share(slot).start()
    both(1, 3, far_multiply)
    both(1, 2, near_multiply)
    pass_on(f1, 4)
    both(7, 8, near_part)

    logit_copy = remote(lg, lg_other, l_send, l_recv, sibling)
    logit_copy.start()
    pass_on(a2, 2)
    share_far(3).start()
    share_far(4).start()
    both(3, 7, near_in)
    both(2, 5, near_multiply)
    both(3, 5, far_multiply)
    pass_on(a2, 3)
    share_far(5).start()
    share_far(6).start()
    near_in(7)
    both(5, 7, near_multiply)

    logit_copy.wait()
    raised = jnp.exp(lg[...] + lg_other[...])
    probs = raised / jnp.sum(raised, axis=0, keepdims=True)
    chosen_first = jnp.sum(jnp.where(names == routing[0:1, :], probs, 0.0), axis=0, keepdims=True)
    chosen_second = jnp.sum(jnp.where(names == routing[1:2, :], probs, 0.0), axis=0, keepdims=True)
    packed = jnp.concatenate(
        [base[0:1, :], base[1:2, :], chosen_first, chosen_second, jnp.zeros((124, GROUP), F32)], axis=0
    )
    packed = jnp.transpose(packed)
    at_first, at_second = packed[:, 0:1].astype(jnp.int32), packed[:, 1:2].astype(jnp.int32)
    by_first, by_second = packed[:, 2:3], packed[:, 3:4]

    def weights(start, size):
        columns = lax.broadcasted_iota(jnp.int32, (GROUP, size), 1) + start
        return (
            jnp.where(columns == at_first, by_first, 0.0) + jnp.where(columns == at_second, by_second, 0.0)
        ).astype(BF16)

    cn[...] = weights(0, NR)
    cf[...] = weights(NR, FR)

    both(7, 8, near_multiply)

    def share_hidden(buffer, which):
        return remote(
            buffer.at[0], buffer.at[1], h_send.at[which], h_recv.at[which], sibling
        )

    hn[0] = jax.nn.gelu(acc_n[...], approximate=True).astype(BF16)
    share_hidden(hn, 0).start()
    for slot in range(Z):
        w2_copy(slot).wait()
        w2_share(slot).wait_recv()

    def bn(slot, p):
        block = pl.ds(p * CAP, CAP)
        return remote(
            pn.at[slot, block], rn.at[slot, block], bn_send.at[slot], bn_recv.at[slot], back[p]
        )

    def bn_all(slot):
        block = pl.ds(0, NR - CAP)
        return remote(
            pn.at[slot, block], rn.at[slot, block], bn_send.at[slot], bn_recv.at[slot], sibling
        )

    def second(buffer, slot):
        return (
            jnp.dot(buffer[0], w2[slot, 0:HID, :], preferred_element_type=F32)
            + jnp.dot(buffer[1], w2[slot, HID:2 * HID, :], preferred_element_type=F32)
        ).astype(BF16)

    def near_out(index):
        slot = 7 - index
        terms = second(hn, slot)
        pn[slot] = terms
        rn[slot, SELF * CAP:(SELF + 1) * CAP, :] = terms[SELF * CAP:(SELF + 1) * CAP, :]
        for p in NEAR_ORDER:
            bn(slot, p).start()

    both(5, 7, far_multiply)
    share_hidden(hn, 0).wait_recv()
    both(0, 1, near_out)
    pass_on(a2, 4)
    share_far(7).start()
    both(1, 3, near_out)
    both(7, 8, far_multiply)
    hf[0] = jax.nn.gelu(acc_f[...], approximate=True).astype(BF16)
    share_hidden(hf, 1).start()
    both(3, 5, near_out)
    share_hidden(hf, 1).wait_recv()

    def far_out(index):
        slot = 7 - index
        pf[slot] = second(hf, slot)

    def reduce_copy(own, received, halves, send, recv, step, way, half):
        start, size = halves[half]
        return remote(
            own.at[back_slot(step, way), pl.ds(start, size)], received.at[way, step - 1, pl.ds(start, size)],
            send.at[step - 1, way, half], recv.at[step - 1, way, half], along[way],
        )

    bf = functools.partial(reduce_copy, pf, rf, F_HALF, bf_send, bf_recv)
    bm = functools.partial(reduce_copy, pm, rm, M_HALF, bm_send, bm_recv)

    def reduce_step(transfer, own, received, halves, step):
        for way, half in back_parts_of(step):
            if step > 1 and (way, half) in back_parts_of(step - 1):
                transfer(step - 1, way, half).wait_recv()
                start, size = halves[half]
                slot = back_slot(step, way)
                own[slot, start:start + size, :] = (
                    own[slot, start:start + size, :].astype(F32)
                    + received[way, step - 2, start:start + size, :].astype(F32)
                ).astype(BF16)
            transfer(step, way, half).start()

    def mix(slot):
        bn_all(slot).wait_recv()
        pm[slot] = jnp.dot(cn[...], rn[slot], preferred_element_type=F32).astype(BF16)

    def mix_down(index):
        mix(7 - index)

    both(0, 1, far_out)
    reduce_step(bf, pf, rf, F_HALF, 1)
    both(1, 3, far_out)
    both(0, 1, mix_down)
    reduce_step(bm, pm, rm, M_HALF, 1)
    both(5, 7, near_out)
    reduce_step(bf, pf, rf, F_HALF, 2)
    both(3, 5, far_out)
    both(7, 8, near_out)
    both(1, 3, mix_down)
    reduce_step(bm, pm, rm, M_HALF, 2)
    reduce_step(bf, pf, rf, F_HALF, 3)
    both(5, 8, far_out)
    both(3, 5, mix_down)
    reduce_step(bf, pf, rf, F_HALF, 4)
    reduce_step(bm, pm, rm, M_HALF, 3)
    both(5, 8, mix_down)

    for way, half in back_parts_of(4):
        bf(4, way, half).wait_recv()
    fr[...] = (
        pf[0].astype(F32) + rf[0, 3].astype(F32) + rf[1, 3].astype(F32)
    ).astype(BF16)

    def far_back(p):
        block = pl.ds((p - NEAR) * CAP, CAP)
        return remote(fr.at[block], ra.at[block], ra_send, ra_recv, back[p])

    for p in FAR_ORDER:
        far_back(p).start()
    reduce_step(bm, pm, rm, M_HALF, 4)
    remote(fr, ra, ra_send, ra_recv, sibling).wait_recv()
    far_term[...] = jnp.dot(cf[...], ra[...], preferred_element_type=F32) + pm[0].astype(F32)
    for way, half in back_parts_of(4):
        bm(4, way, half).wait_recv()
    out[...] = (far_term[...] + rm[0, 3].astype(F32) + rm[1, 3].astype(F32)).astype(BF16)

    for step in range(1, 5):
        for way, half in parts_of(step):
            f1(step, way, half).wait_send()
            a2(step, way, half).wait_send()
        for way, half in back_parts_of(step):
            bf(step, way, half).wait_send()
            bm(step, way, half).wait_send()
    remote(far_send.at[pl_all], xf.at[0, 0, pl_all], a1_send, a1_recv, sibling).wait_send()
    remote(fr, ra, ra_send, ra_recv, sibling).wait_send()

    def sent(slot):
        f2_all(slot).wait_send()
        bn_all(slot).wait_send()
        share_near(slot).wait_send()
        share_far(slot).wait_send()

    both(0, Z, sent)
    for slot in range(Z):
        w2_share(slot).wait_send()
    share_hidden(hn, 0).wait_send()
    share_hidden(hf, 1).wait_send()


def layer(tokens, routing, gate_weight, expert_in, expert_out):
    vmem = pl.BlockSpec(memory_space=pltpu.VMEM)
    anywhere = pl.BlockSpec(memory_space=pl.ANY)
    dma = pltpu.SemaphoreType.DMA
    return pl.pallas_call(
        kernel,
        out_shape=jax.ShapeDtypeStruct((GROUP, W), BF16),
        in_specs=[anywhere, vmem, vmem, anywhere, anywhere],
        out_specs=vmem,
        scratch_shapes=[
            pltpu.VMEM((Z, TB, W), BF16),
            pltpu.VMEM((EXPERTS * CAP, GROUP), BF16),
            pltpu.VMEM((Z, NR, W), BF16),
            pltpu.VMEM((FR, W), BF16),
            pltpu.VMEM((Z, 2, NR, W), BF16),
            pltpu.VMEM((Z, 2, FR, W), BF16),
            pltpu.VMEM((NR, HID), F32),
            pltpu.VMEM((FR, HID), F32),
            pltpu.VMEM((Z, 2, W, HID), BF16),
            pltpu.VMEM((Z, 2 * HID, W), BF16),
            pltpu.VMEM((2, NR, HID), BF16),
            pltpu.VMEM((2, FR, HID), BF16),
            pltpu.VMEM((Z, FR, W), BF16),
            pltpu.VMEM((2, 4, FR, W), BF16),
            pltpu.VMEM((Z, NR, W), BF16),
            pltpu.VMEM((Z, NR, W), BF16),
            pltpu.VMEM((Z, GROUP, W), BF16),
            pltpu.VMEM((2, 4, GROUP, W), BF16),
            pltpu.VMEM((FR, W), BF16),
            pltpu.VMEM((FR, W), BF16),
            pltpu.VMEM((GROUP, NR), BF16),
            pltpu.VMEM((GROUP, FR), BF16),
            pltpu.VMEM((EXPERTS, GROUP), F32),
            pltpu.VMEM((EXPERTS, GROUP), F32),
            pltpu.VMEM((8, GROUP), F32),
            pltpu.VMEM((GROUP, W), F32),
            dma, dma((Z, 2)), dma((Z,)), dma((Z,)), dma((Z,)),
            dma((4, 2, 2)), dma((4, 2, 2)), dma, dma, dma((Z,)), dma((Z,)), dma((4, 2, 2)), dma((4, 2, 2)),
            dma((Z,)), dma((Z,)), dma((Z,)), dma((Z,)), dma((2,)), dma((2,)), dma, dma,
            dma((4, 2, 2)), dma((4, 2, 2)), dma((Z,)), dma((Z,)), dma((4, 2, 2)), dma((4, 2, 2)), dma, dma,
        ],
        compiler_params=pltpu.CompilerParams(collective_id=0, has_side_effects=True),
        name="experts",
    )(tokens, routing.T, gate_weight.T, expert_in, expert_out)


def solution(mesh):
    return jax.shard_map(
        layer,
        mesh=mesh,
        in_specs=(
            P("dp", "expert"),
            P("dp", None),
            P("expert", None),
            P("dp", None, "expert"),
            P("dp", "expert", None),
        ),
        out_specs=P("dp", "expert"),
        check_vma=False,
    )
```

```python
import functools

import jax
import jax.numpy as jnp
from jax import lax
from jax.experimental import pallas as pl
from jax.experimental.pallas import tpu as pltpu
from jax.sharding import PartitionSpec as P

MESH = pl.DeviceIdType.MESH
F32 = jnp.float32
BF16 = jnp.bfloat16

X, Y, Z = 4, 4, 8
GROUP, CAP, EXPERTS, W, HID = 256, 48, 16, 256, 512
SHIFTS = [(dx, dy) for dy in (-1, 0, 1) for dx in (-1, 0, 1)]
SHIFTS += [(2, 0), (0, 2), (2, -1), (2, 1), (2, 2), (-1, 2), (1, 2)]
NEAR, FAR, SELF = 11, 5, 4
NR, FR = NEAR * CAP, FAR * CAP
NEAR_ORDER = [1, 3, 7, 5, 9, 10, 0, 8, 2, 6]
FAR_ORDER = [13, 11, 14, 12, 15]
TB = GROUP + EXPERTS
T_HALF = ((0, 128), (128, TB - 128))
F_HALF = ((0, 3 * CAP), (3 * CAP, FR - 3 * CAP))
M_HALF = ((0, 128), (128, 128))


def parts_of(step):
    return ((0, 0), (1, 1)) if step == 4 else ((0, 0), (1, 1), (0, 1), (1, 0))


def back_parts_of(step):
    return ((0, 0), (1, 1)) if step == 1 else ((0, 1), (1, 0), (0, 0), (1, 1))


def offset_of(slot):
    return 4 if slot == 7 else (slot // 2 if slot % 2 == 0 else -((slot + 1) // 2))


def gather_slots(step, way):
    source = 0 if step == 1 else 2 * step - 3 + way
    return source, (7 if step == 4 else 2 * step - 1 + way)


def back_slot(step, way):
    return 7 if step == 1 else 2 * (5 - step) - way


def kernel(
    tokens, routing, gate, w_in, w_out, out,
    tg, assign, near_send, far_send, xn, xf, acc_n, acc_f, w1, w2, hn, hf,
    pf, rf, pn, rn, pm, rm, fr, ra, cn, cf, lg, lg_other, base, far_term,
    tok_sem, w1_sem, w2_sem, w2s_send, w2s_recv,
    f1_send, f1_recv, a1_send, a1_recv, f2_send, f2_recv, a2_send, a2_recv,
    sn_send, sn_recv, sf_send, sf_recv, h_send, h_recv, l_send, l_recv,
    bf_send, bf_recv, bn_send, bn_recv, bm_send, bm_recv, ra_send, ra_recv,
):
    dp = lax.axis_index("dp")
    ex = lax.axis_index("expert")
    gy, gx = lax.div(dp, X), lax.rem(dp, X)
    z, core = lax.div(ex, 2), lax.rem(ex, 2)

    def plane(dx, dy):
        return (lax.rem(gy + dy + Y, Y) * X + lax.rem(gx + dx + X, X), ex)

    def ring(offset):
        return lax.rem(z + offset + Z, Z)

    to = [plane(dx, dy) for dx, dy in SHIFTS]
    back = [plane(-dx, -dy) for dx, dy in SHIFTS]
    along = ((dp, ring(1) * 2 + core), (dp, ring(-1) * 2 + core))
    sibling = (dp, z * 2 + 1 - core)

    def remote(src, dst, send, recv, device):
        return pltpu.make_async_remote_copy(
            src_ref=src, dst_ref=dst, send_sem=send, recv_sem=recv,
            device_id=device, device_id_type=MESH,
        )

    barrier = pltpu.get_barrier_semaphore()
    for device in [to[p] for p in range(EXPERTS) if p != SELF] + [*along, sibling]:
        pl.semaphore_signal(barrier, inc=1, device_id=device, device_id_type=MESH)

    token_copy = pltpu.make_async_copy(tokens, tg.at[0, pl.ds(0, GROUP)], tok_sem)
    token_copy.start()
    tg[0, GROUP:TB, :] = gate[...]

    def w1_copy(slot, side):
        rows = (ring(offset_of(slot)) * 2 + (core if side == 0 else 1 - core)) * W
        return pltpu.make_async_copy(
            w_in.at[0, pl.ds(pl.multiple_of(rows, W), W), :], w1.at[pl.ds((slot * 2 + side) * W, W)], w1_sem
        )

    def w2_columns(slot, side):
        columns = (ring(offset_of(slot)) * 2 + (core if side == 0 else 1 - core)) * W
        return w_out.at[0, :, pl.ds(pl.multiple_of(columns, W), W)]

    def w2_copy(slot):
        return pltpu.make_async_copy(w2_columns(slot, 0), w2.at[slot, pl.ds(0, HID)], w2_sem)

    def w2_share(slot):
        return remote(
            w2_columns(slot, 1), w2.at[slot, pl.ds(HID, HID)], w2s_send, w2s_recv, sibling
        )

    def f1(step, way, half):
        source, target = gather_slots(step, way)
        start, size = T_HALF[half]
        return remote(
            tg.at[source, pl.ds(start, size)], tg.at[target, pl.ds(start, size)],
            f1_send, f1_recv.at[step - 1, way, half], along[way],
        )

    def a1(p):
        block = pl.ds((p - NEAR) * CAP, CAP)
        return remote(far_send.at[block], xf.at[0, 0, block], a1_send, a1_recv, to[p])

    def f2(slot, p):
        block = pl.ds(p * CAP, CAP)
        return remote(
            near_send.at[slot, block], xn.at[slot, 0, block], f2_send, f2_recv.at[slot], to[p]
        )

    def f2_all(slot):
        block = pl.ds(0, NR - CAP)
        return remote(
            near_send.at[slot, block], xn.at[slot, 0, block], f2_send, f2_recv.at[slot], sibling
        )

    def a2(step, way, half):
        source, target = gather_slots(step, way)
        start, size = F_HALF[half]
        return remote(
            xf.at[source, 0, pl.ds(start, size)], xf.at[target, 0, pl.ds(start, size)],
            a2_send, a2_recv.at[step - 1, way, half], along[way],
        )

    def share_near(slot):
        return remote(xn.at[slot, 0], xn.at[slot, 1], sn_send, sn_recv.at[slot], sibling)

    def share_far(slot):
        return remote(xf.at[slot, 0], xf.at[slot, 1], sf_send, sf_recv.at[slot], sibling)

    def send_near(slot):
        for p in NEAR_ORDER:
            f2(slot, p).start()

    def pass_on(transfer, step):
        for way, half in parts_of(step):
            transfer(step, way, half).wait_recv()
            if step < 4 and (way, half) in parts_of(step + 1):
                transfer(step + 1, way, half).start()

    names = lax.broadcasted_iota(jnp.int32, (EXPERTS, GROUP), 0)
    sx = (lax.rem(names, X) - gx + 1 + X) & 3
    sy = (lax.div(names, X) - gy + 1 + Y) & 3
    place = sy * 3 + sx
    for p in range(9, EXPERTS):
        dx, dy = SHIFTS[p]
        place = jnp.where((sx == dx + 1) & (sy == dy + 1), p, place)
    place = (place * CAP).astype(F32)
    first = (names == routing[0:1, :]).astype(F32)
    second = (names == routing[1:2, :]).astype(F32)
    earlier = lax.broadcasted_iota(jnp.int32, (GROUP, GROUP), 0)
    later = lax.broadcasted_iota(jnp.int32, (GROUP, GROUP), 1)
    upper = (earlier < later).astype(F32).astype(BF16)
    before_first = jnp.dot(first.astype(BF16), upper, preferred_element_type=F32)
    before_second = jnp.dot(second.astype(BF16), upper, preferred_element_type=F32)
    before_second = before_second + jnp.sum(first, axis=1, keepdims=True)
    row_first = jnp.sum(first * (place + before_first), axis=0, keepdims=True)
    row_second = jnp.sum(second * (place + before_second), axis=0, keepdims=True)
    rows = lax.broadcasted_iota(jnp.int32, (EXPERTS * CAP, GROUP), 0)
    hit = (rows == row_first.astype(jnp.int32)) | (rows == row_second.astype(jnp.int32))
    assign[...] = hit.astype(F32).astype(BF16)
    base[0:1, :] = row_first
    base[1:2, :] = row_second
    lg[...] = jnp.zeros_like(lg)

    token_copy.wait()
    pl.semaphore_wait(barrier, 18)
    for way, half in parts_of(1):
        f1(1, way, half).start()
    far_send[...] = jnp.dot(
        assign[NR:, :], tg[0, 0:GROUP, :], preferred_element_type=F32
    ).astype(BF16)

    def dispatch_near(slot):
        rows_of = jnp.dot(assign[0:NR, :], tg[slot, 0:GROUP, :], preferred_element_type=F32).astype(BF16)
        near_send[slot] = rows_of
        xn[slot, 0, SELF * CAP:(SELF + 1) * CAP, :] = rows_of[SELF * CAP:(SELF + 1) * CAP, :]
        lg[...] += lax.dot_general(
            tg[slot, GROUP:TB, :], tg[slot, 0:GROUP, :], (((1,), (1,)), ((), ())), preferred_element_type=F32
        )

    for p in FAR_ORDER:
        a1(p).start()
    dispatch_near(0)
    send_near(0)
    for slot in range(Z):
        for side in range(2):
            w1_copy(slot, side).start()
    for slot in range(Z):
        w2_copy(slot).start()

    acc_n[...] = jnp.zeros_like(acc_n)
    acc_f[...] = jnp.zeros_like(acc_f)

    def both(lower, upper, work):
        lax.fori_loop(lower, upper, lambda slot, carry: (work(slot), carry)[1], 0)

    def near_part(slot):
        dispatch_near(slot)
        send_near(slot)

    def multiply(rows_of, total, slot, count):
        columns = [rows_of[slot + i, side] for i in range(count) for side in range(2)]
        depth = 2 * W * count
        start = pl.multiple_of(slot * 2 * W, 2 * W)
        total[...] += jnp.dot(
            jnp.concatenate(columns, axis=1), w1[pl.ds(start, depth), :], preferred_element_type=F32
        )

    def near_in(slot):
        f2_all(slot).wait_recv()
        share_near(slot).start()

    def near_multiply(slot, count=1):
        for i in range(count):
            share_near(slot + i).wait_recv()
        multiply(xn, acc_n, slot, count)

    def far_multiply(slot, count=1):
        for i in range(count):
            share_far(slot + i).wait_recv()
        multiply(xf, acc_f, slot, count)

    def w2_shares(lower, upper):
        for slot in range(lower, upper):
            w2_share(slot).start()

    def w2_shares(lower, upper):
        for slot in range(lower, upper):
            w2_share(slot).start()

    pass_on(f1, 1)
    both(1, 3, near_part)
    w2_shares(0, 2)
    pl_all = pl.ds(0, FR)
    remote(far_send.at[pl_all], xf.at[0, 0, pl_all], a1_send, a1_recv, sibling).wait_recv()
    for way, half in parts_of(1):
        a2(1, way, half).start()
    share_far(0).start()
    pass_on(f1, 2)
    both(3, 5, near_part)
    near_in(0)
    w2_shares(2, 4)
    pltpu.make_async_copy(w_in.at[0], w1, w1_sem).wait()
    pass_on(a2, 1)
    share_far(1).start()
    share_far(2).start()
    pass_on(f1, 3)
    both(5, 7, near_part)
    both(1, 3, near_in)
    w2_shares(4, 6)
    far_multiply(0, 1)
    near_multiply(0, 1)
    pass_on(a2, 2)
    share_far(3).start()
    share_far(4).start()
    pass_on(f1, 4)
    both(7, 8, near_part)
    w2_shares(6, 8)

    logit_copy = remote(lg, lg_other, l_send, l_recv, sibling)
    logit_copy.start()
    both(3, 5, near_in)
    far_multiply(1, 2)
    pass_on(a2, 3)
    share_far(5).start()
    share_far(6).start()
    near_multiply(1, 2)
    both(5, 7, near_in)
    far_multiply(3, 2)
    near_multiply(3, 2)
    pass_on(a2, 4)
    share_far(7).start()
    near_in(7)
    near_multiply(5, 2)
    near_multiply(7, 1)

    def share_hidden(buffer, which):
        return remote(
            buffer.at[0], buffer.at[1], h_send.at[which], h_recv.at[which], sibling
        )

    hn[0] = jax.nn.gelu(acc_n[...], approximate=True).astype(BF16)
    share_hidden(hn, 0).start()
    far_multiply(5, 2)
    far_multiply(7, 1)
    hf[0] = jax.nn.gelu(acc_f[...], approximate=True).astype(BF16)
    share_hidden(hf, 1).start()
    own_half, other_half = w2.at[:, pl.ds(0, HID)], w2.at[:, pl.ds(HID, HID)]
    pltpu.make_async_copy(own_half, own_half, w2_sem).wait()
    w2_all = remote(own_half, other_half, w2s_send, w2s_recv, sibling)
    w2_all.wait_recv()

    def bn(slot, p):
        block = pl.ds(p * CAP, CAP)
        return remote(
            pn.at[slot, block], rn.at[slot, block], bn_send, bn_recv.at[slot], back[p]
        )

    def bn_all(slot):
        block = pl.ds(0, NR - CAP)
        return remote(
            pn.at[slot, block], rn.at[slot, block], bn_send, bn_recv.at[slot], sibling
        )

    def second(buffer, slot):
        return jnp.dot(
            jnp.concatenate([buffer[0], buffer[1]], axis=1), w2[slot], preferred_element_type=F32
        ).astype(BF16)

    def near_out(index):
        slot = 7 - index
        terms = second(hn, slot)
        pn[slot] = terms
        rn[slot, SELF * CAP:(SELF + 1) * CAP, :] = terms[SELF * CAP:(SELF + 1) * CAP, :]
        for p in NEAR_ORDER:
            bn(slot, p).start()

    def far_out(index):
        slot = 7 - index
        pf[slot] = second(hf, slot)

    def reduce_copy(own, received, halves, send, recv, step, way, half):
        start, size = halves[half]
        return remote(
            own.at[back_slot(step, way), pl.ds(start, size)], received.at[way, step - 1, pl.ds(start, size)],
            send, recv.at[step - 1, way, half], along[way],
        )

    bf = functools.partial(reduce_copy, pf, rf, F_HALF, bf_send, bf_recv)
    bm = functools.partial(reduce_copy, pm, rm, M_HALF, bm_send, bm_recv)

    def reduce_step(transfer, own, received, halves, step, chosen=None):
        for way, half in chosen or back_parts_of(step):
            if step > 1 and (way, half) in back_parts_of(step - 1):
                transfer(step - 1, way, half).wait_recv()
                start, size = halves[half]
                slot = back_slot(step, way)
                own[slot, start:start + size, :] = (
                    own[slot, start:start + size, :].astype(F32)
                    + received[way, step - 2, start:start + size, :].astype(F32)
                ).astype(BF16)
            transfer(step, way, half).start()

    fresh, held = ((0, 1), (1, 0)), ((0, 0), (1, 1))

    def mix(slot):
        bn_all(slot).wait_recv()
        pm[slot] = jnp.dot(cn[...], rn[slot], preferred_element_type=F32).astype(BF16)

    def mix_down(index):
        mix(7 - index)

    share_hidden(hn, 0).wait_recv()
    both(0, 1, near_out)
    share_hidden(hf, 1).wait_recv()
    both(0, 1, far_out)
    reduce_step(bf, pf, rf, F_HALF, 1)
    both(1, 2, near_out)
    both(1, 3, far_out)
    reduce_step(bf, pf, rf, F_HALF, 2, fresh)
    both(2, 3, near_out)
    logit_copy.wait()
    raised = jnp.exp(lg[...] + lg_other[...])
    probs = raised / jnp.sum(raised, axis=0, keepdims=True)
    chosen_first = jnp.sum(jnp.where(names == routing[0:1, :], probs, 0.0), axis=0, keepdims=True)
    chosen_second = jnp.sum(jnp.where(names == routing[1:2, :], probs, 0.0), axis=0, keepdims=True)
    packed = jnp.concatenate(
        [base[0:1, :], base[1:2, :], chosen_first, chosen_second, jnp.zeros((124, GROUP), F32)], axis=0
    )
    packed = jnp.transpose(packed)
    at_first, at_second = packed[:, 0:1].astype(jnp.int32), packed[:, 1:2].astype(jnp.int32)
    by_first, by_second = packed[:, 2:3], packed[:, 3:4]

    def weights(start, size):
        columns = lax.broadcasted_iota(jnp.int32, (GROUP, size), 1) + start
        return (
            jnp.where(columns == at_first, by_first, 0.0) + jnp.where(columns == at_second, by_second, 0.0)
        ).astype(BF16)

    cn[...] = weights(0, NR)
    cf[...] = weights(NR, FR)

    both(3, 4, near_out)
    both(3, 5, far_out)
    reduce_step(bf, pf, rf, F_HALF, 2, held)
    both(4, 5, near_out)
    reduce_step(bf, pf, rf, F_HALF, 3, fresh)
    both(5, 7, far_out)
    both(5, 6, near_out)
    both(0, 1, mix_down)
    reduce_step(bm, pm, rm, M_HALF, 1)
    both(6, 7, near_out)
    reduce_step(bf, pf, rf, F_HALF, 3, held)
    reduce_step(bf, pf, rf, F_HALF, 4, fresh)
    both(1, 2, mix_down)
    reduce_step(bm, pm, rm, M_HALF, 2, fresh[:1])
    both(7, 8, near_out)
    both(2, 3, mix_down)
    reduce_step(bm, pm, rm, M_HALF, 2, fresh[1:])
    both(7, 8, far_out)
    reduce_step(bm, pm, rm, M_HALF, 2, held)
    reduce_step(bf, pf, rf, F_HALF, 4, held)
    both(3, 5, mix_down)
    reduce_step(bm, pm, rm, M_HALF, 3)

    for way, half in back_parts_of(4):
        bf(4, way, half).wait_recv()
    fr[...] = (
        pf[0].astype(F32) + rf[0, 3].astype(F32) + rf[1, 3].astype(F32)
    ).astype(BF16)

    def far_back(p):
        block = pl.ds((p - NEAR) * CAP, CAP)
        return remote(fr.at[block], ra.at[block], ra_send, ra_recv, back[p])

    for p in FAR_ORDER:
        far_back(p).start()
    both(5, 7, mix_down)
    reduce_step(bm, pm, rm, M_HALF, 4)
    both(7, 8, mix_down)
    remote(fr, ra, ra_send, ra_recv, sibling).wait_recv()
    far_term[...] = jnp.dot(cf[...], ra[...], preferred_element_type=F32) + pm[0].astype(F32)
    for way, half in back_parts_of(4):
        bm(4, way, half).wait_recv()
    out[...] = (far_term[...] + rm[0, 3].astype(F32) + rm[1, 3].astype(F32)).astype(BF16)

    def sent(ref, semaphore):
        remote(ref, ref, semaphore, semaphore, sibling).wait_send()

    ring_blocks, most = pl.ds(0, Z - 1), pl.ds(0, NR - CAP)
    sent(tg.at[ring_blocks], f1_send)
    sent(far_send, a1_send)
    sent(near_send.at[:, most], f2_send)
    sent(xf.at[ring_blocks, 0], a2_send)
    sent(xn.at[:, 0], sn_send)
    sent(xf.at[:, 0], sf_send)
    sent(pf.at[ring_blocks], bf_send)
    sent(pm.at[ring_blocks], bm_send)
    sent(pn.at[:, most], bn_send)
    sent(fr, ra_send)
    w2_all.wait_send()
    share_hidden(hn, 0).wait_send()
    share_hidden(hf, 1).wait_send()


def layer(tokens, routing, gate_weight, expert_in, expert_out):
    vmem = pl.BlockSpec(memory_space=pltpu.VMEM)
    anywhere = pl.BlockSpec(memory_space=pl.ANY)
    dma = pltpu.SemaphoreType.DMA
    return pl.pallas_call(
        kernel,
        out_shape=jax.ShapeDtypeStruct((GROUP, W), BF16),
        in_specs=[anywhere, vmem, vmem, anywhere, anywhere],
        out_specs=vmem,
        scratch_shapes=[
            pltpu.VMEM((Z, TB, W), BF16),
            pltpu.VMEM((EXPERTS * CAP, GROUP), BF16),
            pltpu.VMEM((Z, NR, W), BF16),
            pltpu.VMEM((FR, W), BF16),
            pltpu.VMEM((Z, 2, NR, W), BF16),
            pltpu.VMEM((Z, 2, FR, W), BF16),
            pltpu.VMEM((NR, HID), F32),
            pltpu.VMEM((FR, HID), F32),
            pltpu.VMEM((Z * 2 * W, HID), BF16),
            pltpu.VMEM((Z, 2 * HID, W), BF16),
            pltpu.VMEM((2, NR, HID), BF16),
            pltpu.VMEM((2, FR, HID), BF16),
            pltpu.VMEM((Z, FR, W), BF16),
            pltpu.VMEM((2, 4, FR, W), BF16),
            pltpu.VMEM((Z, NR, W), BF16),
            pltpu.VMEM((Z, NR, W), BF16),
            pltpu.VMEM((Z, GROUP, W), BF16),
            pltpu.VMEM((2, 4, GROUP, W), BF16),
            pltpu.VMEM((FR, W), BF16),
            pltpu.VMEM((FR, W), BF16),
            pltpu.VMEM((GROUP, NR), BF16),
            pltpu.VMEM((GROUP, FR), BF16),
            pltpu.VMEM((EXPERTS, GROUP), F32),
            pltpu.VMEM((EXPERTS, GROUP), F32),
            pltpu.VMEM((8, GROUP), F32),
            pltpu.VMEM((GROUP, W), F32),
            dma, dma, dma, dma, dma,
            dma, dma((4, 2, 2)), dma, dma, dma, dma((Z,)), dma, dma((4, 2, 2)),
            dma, dma((Z,)), dma, dma((Z,)), dma((2,)), dma((2,)), dma, dma,
            dma, dma((4, 2, 2)), dma, dma((Z,)), dma, dma((4, 2, 2)), dma, dma,
        ],
        compiler_params=pltpu.CompilerParams(collective_id=0, has_side_effects=True),
        name="experts",
    )(tokens, routing.T, gate_weight.T, expert_in, expert_out)


def solution(mesh):
    return jax.shard_map(
        layer,
        mesh=mesh,
        in_specs=(
            P("dp", "expert"),
            P("dp", None),
            P("expert", None),
            P("dp", None, "expert"),
            P("dp", "expert", None),
        ),
        out_specs=P("dp", "expert"),
        check_vma=False,
    )
```

```python
import functools

import jax
import jax.numpy as jnp
from jax import lax
from jax.experimental import pallas as pl
from jax.experimental.pallas import tpu as pltpu
from jax.sharding import PartitionSpec as P

MESH = pl.DeviceIdType.MESH
F32 = jnp.float32
BF16 = jnp.bfloat16

X, Y, Z = 4, 4, 8
GROUP, CAP, EXPERTS, W, HID = 256, 48, 16, 256, 512
SHIFTS = [(dx, dy) for dy in (-1, 0, 1) for dx in (-1, 0, 1)]
SHIFTS += [(2, 0), (0, 2), (2, -1), (2, 1), (2, 2), (-1, 2), (1, 2)]
NEAR, FAR, SELF = 11, 5, 4
NR, FR = NEAR * CAP, FAR * CAP
NEAR_ORDER = [1, 3, 7, 5, 9, 10, 0, 8, 2, 6]
FAR_ORDER = [13, 11, 14, 12, 15]
TB = GROUP + EXPERTS
T_HALF = ((0, 128), (128, TB - 128))
F_HALF = ((0, 3 * CAP), (3 * CAP, FR - 3 * CAP))
M_HALF = ((0, 128), (128, 128))


def parts_of(step):
    return ((0, 0), (1, 1)) if step == 4 else ((0, 0), (1, 1), (0, 1), (1, 0))


def back_parts_of(step):
    return ((0, 0), (1, 1)) if step == 1 else ((0, 1), (1, 0), (0, 0), (1, 1))


def offset_of(slot):
    return 4 if slot == 7 else (slot // 2 if slot % 2 == 0 else -((slot + 1) // 2))


def gather_slots(step, way):
    source = 0 if step == 1 else 2 * step - 3 + way
    return source, (7 if step == 4 else 2 * step - 1 + way)


def back_slot(step, way):
    return 7 if step == 1 else 2 * (5 - step) - way


def kernel(
    tokens, picks, gate, w_in, w_out, out,
    tg, assign, near_send, far_send, xn, xf, acc_n, acc_f, w1, w2, hn, hf,
    pf, rf, pn, rn, pm, rm, fr, ra, cn, cf, lg, lg_other, base, far_term, routing,
    tok_sem, gate_sem, picks_sem, w1_sem, w2_sem, w2s_send, w2s_recv,
    f1_send, f1_recv, a1_send, a1_recv, f2_send, f2_recv, a2_send, a2_recv,
    sn_send, sn_recv, sf_send, sf_recv, h_send, h_recv, l_send, l_recv,
    bf_send, bf_recv, bn_send, bn_recv, bm_send, bm_recv, ra_send, ra_recv,
):
    dp = lax.axis_index("dp")
    ex = lax.axis_index("expert")
    gy, gx = lax.div(dp, X), lax.rem(dp, X)
    z, core = lax.div(ex, 2), lax.rem(ex, 2)

    def plane(dx, dy):
        return (lax.rem(gy + dy + Y, Y) * X + lax.rem(gx + dx + X, X), ex)

    def ring(offset):
        return lax.rem(z + offset + Z, Z)

    to = [plane(dx, dy) for dx, dy in SHIFTS]
    back = [plane(-dx, -dy) for dx, dy in SHIFTS]
    along = ((dp, ring(1) * 2 + 1 - core), (dp, ring(-1) * 2 + 1 - core))
    sibling = (dp, z * 2 + 1 - core)

    def remote(src, dst, send, recv, device):
        return pltpu.make_async_remote_copy(
            src_ref=src, dst_ref=dst, send_sem=send, recv_sem=recv,
            device_id=device, device_id_type=MESH,
        )

    barrier = pltpu.get_barrier_semaphore()
    for device in [to[p] for p in range(EXPERTS) if p != SELF] + [*along, sibling]:
        pl.semaphore_signal(barrier, inc=1, device_id=device, device_id_type=MESH)

    picks_copy = pltpu.make_async_copy(picks, routing, picks_sem)
    picks_copy.start()
    token_copy = pltpu.make_async_copy(tokens, tg.at[0, pl.ds(0, GROUP)], tok_sem)
    token_copy.start()
    gate_copy = pltpu.make_async_copy(gate, tg.at[0, pl.ds(GROUP, EXPERTS)], gate_sem)
    gate_copy.start()
    picks_copy.wait()

    def block_of(slot, side):
        offset = offset_of(slot)
        return ring(offset) * 2 + (core if (offset + side) % 2 == 0 else 1 - core)

    def w1_copy(slot, side):
        rows = block_of(slot, side) * W
        return pltpu.make_async_copy(
            w_in.at[0, pl.ds(pl.multiple_of(rows, W), W), :], w1.at[pl.ds((slot * 2 + side) * W, W)], w1_sem
        )

    def w2_columns(slot, side):
        columns = block_of(slot, side) * W
        return w_out.at[0, :, pl.ds(pl.multiple_of(columns, W), W)]

    def w2_copy(slot):
        return pltpu.make_async_copy(w2_columns(slot, 0), w2.at[slot, pl.ds(0, HID)], w2_sem)

    def w2_share(slot):
        return remote(
            w2_columns(slot, 1), w2.at[slot, pl.ds(HID, HID)], w2s_send, w2s_recv, sibling
        )

    def f1(step, way, half):
        source, target = gather_slots(step, way)
        start, size = T_HALF[half]
        return remote(
            tg.at[source, pl.ds(start, size)], tg.at[target, pl.ds(start, size)],
            f1_send, f1_recv.at[step - 1, way, half], along[way],
        )

    def a1(p):
        block = pl.ds((p - NEAR) * CAP, CAP)
        return remote(far_send.at[block], xf.at[0, 0, block], a1_send, a1_recv, to[p])

    def f2(slot, p):
        block = pl.ds(p * CAP, CAP)
        return remote(
            near_send.at[slot, block], xn.at[slot, 0, block], f2_send, f2_recv.at[slot], to[p]
        )

    def f2_all(slot):
        block = pl.ds(0, NR - CAP)
        return remote(
            near_send.at[slot, block], xn.at[slot, 0, block], f2_send, f2_recv.at[slot], sibling
        )

    def a2(step, way, half):
        source, target = gather_slots(step, way)
        start, size = F_HALF[half]
        return remote(
            xf.at[source, 0, pl.ds(start, size)], xf.at[target, 0, pl.ds(start, size)],
            a2_send, a2_recv.at[step - 1, way, half], along[way],
        )

    def share_near(slot):
        return remote(xn.at[slot, 0], xn.at[slot, 1], sn_send, sn_recv.at[slot], sibling)

    def share_far(slot):
        return remote(xf.at[slot, 0], xf.at[slot, 1], sf_send, sf_recv.at[slot], sibling)

    def send_near(slot):
        for p in NEAR_ORDER:
            f2(slot, p).start()

    def pass_on(transfer, step):
        for way, half in parts_of(step):
            transfer(step, way, half).wait_recv()
            if step < 4 and (way, half) in parts_of(step + 1):
                transfer(step + 1, way, half).start()

    names = lax.broadcasted_iota(jnp.int32, (EXPERTS, GROUP), 0)
    sx = (lax.rem(names, X) - gx + 1 + X) & 3
    sy = (lax.div(names, X) - gy + 1 + Y) & 3
    place = sy * 3 + sx
    for p in range(9, EXPERTS):
        dx, dy = SHIFTS[p]
        place = jnp.where((sx == dx + 1) & (sy == dy + 1), p, place)
    place = (place * CAP).astype(F32)
    first = (names == routing[0:1, :]).astype(F32)
    second = (names == routing[1:2, :]).astype(F32)
    earlier = lax.broadcasted_iota(jnp.int32, (GROUP, GROUP), 0)
    later = lax.broadcasted_iota(jnp.int32, (GROUP, GROUP), 1)
    upper = (earlier < later).astype(F32).astype(BF16)
    before_first = jnp.dot(first.astype(BF16), upper, preferred_element_type=F32)
    before_second = jnp.dot(second.astype(BF16), upper, preferred_element_type=F32)
    before_second = before_second + jnp.sum(first, axis=1, keepdims=True)
    row_first = jnp.sum(first * (place + before_first), axis=0, keepdims=True)
    row_second = jnp.sum(second * (place + before_second), axis=0, keepdims=True)
    rows = lax.broadcasted_iota(jnp.int32, (EXPERTS * CAP, GROUP), 0)
    hit = (rows == row_first.astype(jnp.int32)) | (rows == row_second.astype(jnp.int32))
    assign[...] = hit.astype(F32).astype(BF16)
    base[0:1, :] = row_first
    base[1:2, :] = row_second
    lg[...] = jnp.zeros_like(lg)

    token_copy.wait()
    gate_copy.wait()
    pl.semaphore_wait(barrier, 18)
    for way, half in parts_of(1):
        f1(1, way, half).start()
    far_send[...] = jnp.dot(
        assign[NR:, :], tg[0, 0:GROUP, :], preferred_element_type=F32
    ).astype(BF16)

    def dispatch_near(slot):
        rows_of = jnp.dot(assign[0:NR, :], tg[slot, 0:GROUP, :], preferred_element_type=F32).astype(BF16)
        near_send[slot] = rows_of
        xn[slot, 0, SELF * CAP:(SELF + 1) * CAP, :] = rows_of[SELF * CAP:(SELF + 1) * CAP, :]
        lg[...] += lax.dot_general(
            tg[slot, GROUP:TB, :], tg[slot, 0:GROUP, :], (((1,), (1,)), ((), ())), preferred_element_type=F32
        )

    for p in FAR_ORDER:
        a1(p).start()
    dispatch_near(0)
    send_near(0)
    for slot in range(Z):
        for side in range(2):
            w1_copy(slot, side).start()
    for slot in range(Z):
        w2_copy(slot).start()

    acc_n[...] = jnp.zeros_like(acc_n)
    acc_f[...] = jnp.zeros_like(acc_f)

    def both(lower, upper, work):
        lax.fori_loop(lower, upper, lambda slot, carry: (work(slot), carry)[1], 0)

    def near_part(slot):
        dispatch_near(slot)
        send_near(slot)

    def multiply(rows_of, total, slot, count):
        columns = [rows_of[slot + i, side] for i in range(count) for side in range(2)]
        depth = 2 * W * count
        start = pl.multiple_of(slot * 2 * W, 2 * W)
        total[...] += jnp.dot(
            jnp.concatenate(columns, axis=1), w1[pl.ds(start, depth), :], preferred_element_type=F32
        )

    def near_in(slot):
        f2_all(slot).wait_recv()
        share_near(slot).start()

    def near_multiply(slot, count=1):
        for i in range(count):
            share_near(slot + i).wait_recv()
        multiply(xn, acc_n, slot, count)

    def far_multiply(slot, count=1):
        for i in range(count):
            share_far(slot + i).wait_recv()
        multiply(xf, acc_f, slot, count)

    def w2_shares(lower, upper):
        for slot in range(lower, upper):
            w2_share(slot).start()

    for slot in range(4):
        w2_share(slot).start()
    pass_on(f1, 1)
    both(1, 3, near_part)
    for slot in range(4, Z):
        w2_share(slot).start()
    pl_all = pl.ds(0, FR)
    remote(far_send.at[pl_all], xf.at[0, 0, pl_all], a1_send, a1_recv, sibling).wait_recv()
    for way, half in parts_of(1):
        a2(1, way, half).start()
    share_far(0).start()
    pass_on(f1, 2)
    both(3, 5, near_part)
    near_in(0)
    pltpu.make_async_copy(w_in.at[0], w1, w1_sem).wait()
    pass_on(a2, 1)
    share_far(1).start()
    share_far(2).start()
    pass_on(f1, 3)
    both(5, 7, near_part)
    both(1, 3, near_in)
    far_multiply(0, 1)
    near_multiply(0, 1)
    pass_on(a2, 2)
    share_far(3).start()
    share_far(4).start()
    pass_on(f1, 4)
    both(7, 8, near_part)

    logit_copy = remote(lg, lg_other, l_send, l_recv, sibling)
    logit_copy.start()
    both(3, 5, near_in)
    far_multiply(1, 2)
    pass_on(a2, 3)
    share_far(5).start()
    share_far(6).start()
    near_multiply(1, 2)
    both(5, 7, near_in)
    far_multiply(3, 2)
    near_multiply(3, 2)
    pass_on(a2, 4)
    share_far(7).start()
    near_in(7)
    far_multiply(5, 2)
    near_multiply(5, 2)
    far_multiply(7, 1)

    def share_hidden(buffer, which):
        return remote(
            buffer.at[:, pl.ds(0, HID)], buffer.at[:, pl.ds(HID, HID)], h_send.at[which], h_recv.at[which], sibling,
        )

    hf[:, 0:HID] = jax.nn.gelu(acc_f[...], approximate=True).astype(BF16)
    share_hidden(hf, 1).start()
    near_multiply(7, 1)
    hn[:, 0:HID] = jax.nn.gelu(acc_n[...], approximate=True).astype(BF16)
    share_hidden(hn, 0).start()
    own_half, other_half = w2.at[:, pl.ds(0, HID)], w2.at[:, pl.ds(HID, HID)]
    pltpu.make_async_copy(own_half, own_half, w2_sem).wait()
    w2_all = remote(own_half, other_half, w2s_send, w2s_recv, sibling)
    w2_all.wait_recv()

    def bn(slot, p):
        block = pl.ds(p * CAP, CAP)
        return remote(
            pn.at[slot, block], rn.at[slot, block], bn_send, bn_recv.at[slot], back[p]
        )

    def bn_all(slot):
        block = pl.ds(0, NR - CAP)
        return remote(
            pn.at[slot, block], rn.at[slot, block], bn_send, bn_recv.at[slot], sibling
        )

    def second(buffer, slot):
        return jnp.dot(buffer[...], w2[slot], preferred_element_type=F32).astype(BF16)

    def near_out(index):
        slot = 7 - index
        terms = second(hn, slot)
        pn[slot] = terms
        rn[slot, SELF * CAP:(SELF + 1) * CAP, :] = terms[SELF * CAP:(SELF + 1) * CAP, :]
        for p in NEAR_ORDER:
            bn(slot, p).start()

    def far_out(index):
        slot = 7 - index
        pf[slot] = second(hf, slot)

    def reduce_copy(own, received, halves, send, recv, step, way, half):
        start, size = halves[half]
        return remote(
            own.at[back_slot(step, way), pl.ds(start, size)], received.at[way, step - 1, pl.ds(start, size)],
            send, recv.at[step - 1, way, half], along[way],
        )

    bf = functools.partial(reduce_copy, pf, rf, F_HALF, bf_send, bf_recv)
    bm = functools.partial(reduce_copy, pm, rm, M_HALF, bm_send, bm_recv)

    def reduce_step(transfer, own, received, halves, step, chosen=None):
        for way, half in chosen or back_parts_of(step):
            if step > 1 and (way, half) in back_parts_of(step - 1):
                transfer(step - 1, way, half).wait_recv()
                start, size = halves[half]
                slot = back_slot(step, way)
                own[slot, start:start + size, :] = (
                    own[slot, start:start + size, :].astype(F32)
                    + received[way, step - 2, start:start + size, :].astype(F32)
                ).astype(BF16)
            transfer(step, way, half).start()

    fresh, held = ((0, 1), (1, 0)), ((0, 0), (1, 1))

    def mix(slot):
        bn_all(slot).wait_recv()
        pm[slot] = jnp.dot(cn[...], rn[slot], preferred_element_type=F32).astype(BF16)

    def mix_down(index):
        mix(7 - index)

    share_hidden(hf, 1).wait_recv()
    both(0, 1, far_out)
    reduce_step(bf, pf, rf, F_HALF, 1)
    both(1, 3, far_out)
    reduce_step(bf, pf, rf, F_HALF, 2, fresh)
    share_hidden(hn, 0).wait_recv()
    both(0, 2, near_out)
    both(2, 3, near_out)
    logit_copy.wait()
    raised = jnp.exp(lg[...] + lg_other[...])
    probs = raised / jnp.sum(raised, axis=0, keepdims=True)
    chosen_first = jnp.sum(jnp.where(names == routing[0:1, :], probs, 0.0), axis=0, keepdims=True)
    chosen_second = jnp.sum(jnp.where(names == routing[1:2, :], probs, 0.0), axis=0, keepdims=True)
    packed = jnp.concatenate(
        [base[0:1, :], base[1:2, :], chosen_first, chosen_second, jnp.zeros((124, GROUP), F32)], axis=0
    )
    packed = jnp.transpose(packed)
    at_first, at_second = packed[:, 0:1].astype(jnp.int32), packed[:, 1:2].astype(jnp.int32)
    by_first, by_second = packed[:, 2:3], packed[:, 3:4]

    def weights(start, size):
        columns = lax.broadcasted_iota(jnp.int32, (GROUP, size), 1) + start
        return (
            jnp.where(columns == at_first, by_first, 0.0) + jnp.where(columns == at_second, by_second, 0.0)
        ).astype(BF16)

    cn[...] = weights(0, NR)
    cf[...] = weights(NR, FR)

    both(3, 4, near_out)
    both(3, 5, far_out)
    reduce_step(bf, pf, rf, F_HALF, 2, held)
    both(4, 5, near_out)
    reduce_step(bf, pf, rf, F_HALF, 3, fresh)
    both(5, 7, far_out)
    both(5, 6, near_out)
    both(0, 1, mix_down)
    reduce_step(bm, pm, rm, M_HALF, 1)
    both(6, 7, near_out)
    reduce_step(bf, pf, rf, F_HALF, 3, held)
    reduce_step(bf, pf, rf, F_HALF, 4, fresh)
    both(1, 2, mix_down)
    reduce_step(bm, pm, rm, M_HALF, 2, fresh[:1])
    both(7, 8, near_out)
    both(2, 3, mix_down)
    reduce_step(bm, pm, rm, M_HALF, 2, fresh[1:])
    both(7, 8, far_out)
    reduce_step(bm, pm, rm, M_HALF, 2, held)
    reduce_step(bf, pf, rf, F_HALF, 4, held)
    both(3, 5, mix_down)
    reduce_step(bm, pm, rm, M_HALF, 3)

    for way, half in back_parts_of(4):
        bf(4, way, half).wait_recv()
    fr[...] = (
        pf[0].astype(F32) + rf[0, 3].astype(F32) + rf[1, 3].astype(F32)
    ).astype(BF16)

    def far_back(p):
        block = pl.ds((p - NEAR) * CAP, CAP)
        return remote(fr.at[block], ra.at[block], ra_send, ra_recv, back[p])

    for p in FAR_ORDER:
        far_back(p).start()
    both(5, 7, mix_down)
    reduce_step(bm, pm, rm, M_HALF, 4)
    both(7, 8, mix_down)
    remote(fr, ra, ra_send, ra_recv, sibling).wait_recv()
    far_term[...] = jnp.dot(cf[...], ra[...], preferred_element_type=F32) + pm[0].astype(F32)
    for way, half in back_parts_of(4):
        bm(4, way, half).wait_recv()
    out[...] = (far_term[...] + rm[0, 3].astype(F32) + rm[1, 3].astype(F32)).astype(BF16)

    def sent(ref, semaphore):
        remote(ref, ref, semaphore, semaphore, sibling).wait_send()

    ring_blocks, most = pl.ds(0, Z - 1), pl.ds(0, NR - CAP)
    sent(tg.at[ring_blocks], f1_send)
    sent(far_send, a1_send)
    sent(near_send.at[:, most], f2_send)
    sent(xf.at[ring_blocks, 0], a2_send)
    sent(xn.at[:, 0], sn_send)
    sent(xf.at[:, 0], sf_send)
    sent(pf.at[ring_blocks], bf_send)
    sent(pm.at[ring_blocks], bm_send)
    sent(pn.at[:, most], bn_send)
    sent(fr, ra_send)
    w2_all.wait_send()
    share_hidden(hn, 0).wait_send()
    share_hidden(hf, 1).wait_send()


def layer(tokens, routing, gate_weight, expert_in, expert_out):
    vmem = pl.BlockSpec(memory_space=pltpu.VMEM)
    anywhere = pl.BlockSpec(memory_space=pl.ANY)
    dma = pltpu.SemaphoreType.DMA
    return pl.pallas_call(
        kernel,
        out_shape=jax.ShapeDtypeStruct((GROUP, W), BF16),
        in_specs=[anywhere] * 5,
        out_specs=vmem,
        scratch_shapes=[
            pltpu.VMEM((Z, TB, W), BF16),
            pltpu.VMEM((EXPERTS * CAP, GROUP), BF16),
            pltpu.VMEM((Z, NR, W), BF16),
            pltpu.VMEM((FR, W), BF16),
            pltpu.VMEM((Z, 2, NR, W), BF16),
            pltpu.VMEM((Z, 2, FR, W), BF16),
            pltpu.VMEM((NR, HID), F32),
            pltpu.VMEM((FR, HID), F32),
            pltpu.VMEM((Z * 2 * W, HID), BF16),
            pltpu.VMEM((Z, 2 * HID, W), BF16),
            pltpu.VMEM((NR, 2 * HID), BF16),
            pltpu.VMEM((FR, 2 * HID), BF16),
            pltpu.VMEM((Z, FR, W), BF16),
            pltpu.VMEM((2, 4, FR, W), BF16),
            pltpu.VMEM((Z, NR, W), BF16),
            pltpu.VMEM((Z, NR, W), BF16),
            pltpu.VMEM((Z, GROUP, W), BF16),
            pltpu.VMEM((2, 4, GROUP, W), BF16),
            pltpu.VMEM((FR, W), BF16),
            pltpu.VMEM((FR, W), BF16),
            pltpu.VMEM((GROUP, NR), BF16),
            pltpu.VMEM((GROUP, FR), BF16),
            pltpu.VMEM((EXPERTS, GROUP), F32),
            pltpu.VMEM((EXPERTS, GROUP), F32),
            pltpu.VMEM((8, GROUP), F32),
            pltpu.VMEM((GROUP, W), F32),
            pltpu.VMEM((2, GROUP), jnp.int32),
            dma, dma, dma, dma, dma, dma, dma,
            dma, dma((4, 2, 2)), dma, dma, dma, dma((Z,)), dma, dma((4, 2, 2)),
            dma, dma((Z,)), dma, dma((Z,)), dma((2,)), dma((2,)), dma, dma,
            dma, dma((4, 2, 2)), dma, dma((Z,)), dma, dma((4, 2, 2)), dma, dma,
        ],
        compiler_params=pltpu.CompilerParams(collective_id=0, has_side_effects=True),
        name="experts",
    )(tokens, routing.T, gate_weight.T, expert_in, expert_out)


def solution(mesh):
    return jax.shard_map(
        layer,
        mesh=mesh,
        in_specs=(
            P("dp", "expert"),
            P("dp", None),
            P("expert", None),
            P("dp", None, "expert"),
            P("dp", "expert", None),
        ),
        out_specs=P("dp", "expert"),
        check_vma=False,
    )
```

```python
import functools

import jax
import jax.numpy as jnp
from jax import lax
from jax.experimental import pallas as pl
from jax.experimental.pallas import tpu as pltpu
from jax.sharding import PartitionSpec as P

MESH = pl.DeviceIdType.MESH
F32 = jnp.float32
BF16 = jnp.bfloat16

X, Y, Z = 4, 4, 8
GROUP, CAP, EXPERTS, W, HID = 256, 48, 16, 256, 512
SHIFTS = [(dx, dy) for dy in (-1, 0, 1) for dx in (-1, 0, 1)]
SHIFTS += [(2, 0), (0, 2), (2, -1), (2, 1), (2, 2), (-1, 2), (1, 2)]
NEAR, FAR, SELF = 11, 5, 4
NR, FR = NEAR * CAP, FAR * CAP
NEAR_ORDER = [1, 3, 7, 5, 9, 10, 0, 8, 2, 6]
FAR_ORDER = [13, 11, 14, 12, 15]
TB = GROUP + EXPERTS
T_HALF = ((0, 128), (128, TB - 128))
F_HALF = ((0, 3 * CAP), (3 * CAP, FR - 3 * CAP))
M_HALF = ((0, 128), (128, 128))


def parts_of(step):
    return ((0, 0), (1, 1)) if step == 4 else ((0, 0), (1, 1), (0, 1), (1, 0))


def back_parts_of(step):
    return ((0, 0), (1, 1)) if step == 1 else ((0, 1), (1, 0), (0, 0), (1, 1))


def offset_of(slot):
    return 4 if slot == 7 else (slot // 2 if slot % 2 == 0 else -((slot + 1) // 2))


def gather_slots(step, way):
    source = 0 if step == 1 else 2 * step - 3 + way
    return source, (7 if step == 4 else 2 * step - 1 + way)


def back_slot(step, way):
    return 7 if step == 1 else 2 * (5 - step) - way


def kernel(
    tokens, picks, gate, w_in, w_out, out,
    tg, assign, near_send, far_send, xn, xf, acc_n, acc_f, w1, w2, hn, hf,
    pf, rf, pn, rn, pm, rm, fr, ra, cn, cf, lg, lg_other, base, far_term, routing,
    tok_sem, gate_sem, picks_sem, w1_sem, w2_sem, w2s_send, w2s_recv,
    f1_send, f1_recv, a1_send, a1_recv, f2_send, f2_recv, a2_send, a2_recv,
    sn_send, sn_recv, sf_send, sf_recv, h_send, h_recv, l_send, l_recv,
    bf_send, bf_recv, bn_send, bn_recv, bm_send, bm_recv, ra_send, ra_recv,
):
    dp = lax.axis_index("dp")
    ex = lax.axis_index("expert")
    gy, gx = lax.div(dp, X), lax.rem(dp, X)
    z, core = lax.div(ex, 2), lax.rem(ex, 2)

    def plane(dx, dy):
        return (lax.rem(gy + dy + Y, Y) * X + lax.rem(gx + dx + X, X), ex)

    def ring(offset):
        return lax.rem(z + offset + Z, Z)

    to = [plane(dx, dy) for dx, dy in SHIFTS]
    back = [plane(-dx, -dy) for dx, dy in SHIFTS]
    along = ((dp, ring(1) * 2 + 1 - core), (dp, ring(-1) * 2 + 1 - core))
    sibling = (dp, z * 2 + 1 - core)

    def remote(src, dst, send, recv, device):
        return pltpu.make_async_remote_copy(
            src_ref=src, dst_ref=dst, send_sem=send, recv_sem=recv,
            device_id=device, device_id_type=MESH,
        )

    barrier = pltpu.get_barrier_semaphore()
    for device in [to[p] for p in range(EXPERTS) if p != SELF] + [*along, sibling]:
        pl.semaphore_signal(barrier, inc=1, device_id=device, device_id_type=MESH)

    picks_copy = pltpu.make_async_copy(picks, routing, picks_sem)
    picks_copy.start()
    token_copy = pltpu.make_async_copy(tokens, tg.at[0, pl.ds(0, GROUP)], tok_sem)
    token_copy.start()
    gate_copy = pltpu.make_async_copy(gate, tg.at[0, pl.ds(GROUP, EXPERTS)], gate_sem)
    gate_copy.start()
    picks_copy.wait()

    def block_of(slot, side):
        offset = offset_of(slot)
        return ring(offset) * 2 + (core if (offset + side) % 2 == 0 else 1 - core)

    def w1_copy(slot, side):
        rows = block_of(slot, side) * W
        return pltpu.make_async_copy(
            w_in.at[0, pl.ds(pl.multiple_of(rows, W), W), :], w1.at[pl.ds((slot * 2 + side) * W, W)], w1_sem
        )

    def w2_columns(slot, side):
        columns = block_of(slot, side) * W
        return w_out.at[0, :, pl.ds(pl.multiple_of(columns, W), W)]

    def w2_copy(slot):
        return pltpu.make_async_copy(w2_columns(slot, 0), w2.at[slot, pl.ds(0, HID)], w2_sem)

    def w2_share(slot):
        return remote(
            w2_columns(slot, 1), w2.at[slot, pl.ds(HID, HID)], w2s_send, w2s_recv, sibling
        )

    def f1(step, way, half):
        source, target = gather_slots(step, way)
        start, size = T_HALF[half]
        return remote(
            tg.at[source, pl.ds(start, size)], tg.at[target, pl.ds(start, size)],
            f1_send, f1_recv.at[step - 1, way, half], along[way],
        )

    def a1(p):
        block = pl.ds((p - NEAR) * CAP, CAP)
        return remote(far_send.at[block], xf.at[0, 0, block], a1_send, a1_recv, to[p])

    def f2(slot, p):
        block = pl.ds(p * CAP, CAP)
        return remote(
            near_send.at[slot, block], xn.at[slot, 0, block], f2_send, f2_recv.at[slot], to[p]
        )

    def f2_all(slot):
        block = pl.ds(0, NR - CAP)
        return remote(
            near_send.at[slot, block], xn.at[slot, 0, block], f2_send, f2_recv.at[slot], sibling
        )

    def a2(step, way, half):
        source, target = gather_slots(step, way)
        start, size = F_HALF[half]
        return remote(
            xf.at[source, 0, pl.ds(start, size)], xf.at[target, 0, pl.ds(start, size)],
            a2_send, a2_recv.at[step - 1, way, half], along[way],
        )

    def share_near(slot):
        return remote(xn.at[slot, 0], xn.at[slot, 1], sn_send, sn_recv.at[slot], sibling)

    def share_far(slot):
        return remote(xf.at[slot, 0], xf.at[slot, 1], sf_send, sf_recv.at[slot], sibling)

    def send_near(slot):
        for p in NEAR_ORDER:
            f2(slot, p).start()

    def pass_on(transfer, step):
        for way, half in parts_of(step):
            transfer(step, way, half).wait_recv()
            if step < 4 and (way, half) in parts_of(step + 1):
                transfer(step + 1, way, half).start()

    names = lax.broadcasted_iota(jnp.int32, (EXPERTS, GROUP), 0)
    sx = (lax.rem(names, X) - gx + 1 + X) & 3
    sy = (lax.div(names, X) - gy + 1 + Y) & 3
    place = sy * 3 + sx
    for p in range(9, EXPERTS):
        dx, dy = SHIFTS[p]
        place = jnp.where((sx == dx + 1) & (sy == dy + 1), p, place)
    place = (place * CAP).astype(F32)
    first = (names == routing[0:1, :]).astype(F32)
    second = (names == routing[1:2, :]).astype(F32)
    earlier = lax.broadcasted_iota(jnp.int32, (GROUP, GROUP), 0)
    later = lax.broadcasted_iota(jnp.int32, (GROUP, GROUP), 1)
    upper = (earlier < later).astype(F32).astype(BF16)
    before_first = jnp.dot(first.astype(BF16), upper, preferred_element_type=F32)
    before_second = jnp.dot(second.astype(BF16), upper, preferred_element_type=F32)
    before_second = before_second + jnp.sum(first, axis=1, keepdims=True)
    row_first = jnp.sum(first * (place + before_first), axis=0, keepdims=True)
    row_second = jnp.sum(second * (place + before_second), axis=0, keepdims=True)
    rows = lax.broadcasted_iota(jnp.int32, (EXPERTS * CAP, GROUP), 0)
    hit = (rows == row_first.astype(jnp.int32)) | (rows == row_second.astype(jnp.int32))
    assign[...] = hit.astype(F32).astype(BF16)
    base[0:1, :] = row_first
    base[1:2, :] = row_second
    lg[...] = jnp.zeros_like(lg)

    token_copy.wait()
    gate_copy.wait()
    pl.semaphore_wait(barrier, 18)
    for way, half in parts_of(1):
        f1(1, way, half).start()
    far_send[...] = jnp.dot(
        assign[NR:, :], tg[0, 0:GROUP, :], preferred_element_type=F32
    ).astype(BF16)

    def dispatch_near(slot):
        rows_of = jnp.dot(assign[0:NR, :], tg[slot, 0:GROUP, :], preferred_element_type=F32).astype(BF16)
        near_send[slot] = rows_of
        xn[slot, 0, SELF * CAP:(SELF + 1) * CAP, :] = rows_of[SELF * CAP:(SELF + 1) * CAP, :]
        lg[...] += lax.dot_general(
            tg[slot, GROUP:TB, :], tg[slot, 0:GROUP, :], (((1,), (1,)), ((), ())), preferred_element_type=F32
        )

    for p in FAR_ORDER:
        a1(p).start()
    dispatch_near(0)
    send_near(0)
    for slot in range(Z):
        for side in range(2):
            w1_copy(slot, side).start()
    for slot in range(Z):
        w2_copy(slot).start()

    acc_n[...] = jnp.zeros_like(acc_n)
    acc_f[...] = jnp.zeros_like(acc_f)

    def both(lower, upper, work):
        lax.fori_loop(lower, upper, lambda slot, carry: (work(slot), carry)[1], 0)

    def near_part(slot):
        dispatch_near(slot)
        send_near(slot)

    def multiply(rows_of, total, slot, count):
        columns = [rows_of[slot + i, side] for i in range(count) for side in range(2)]
        depth = 2 * W * count
        start = pl.multiple_of(slot * 2 * W, 2 * W)
        total[...] += jnp.dot(
            jnp.concatenate(columns, axis=1), w1[pl.ds(start, depth), :], preferred_element_type=F32
        )

    def near_in(slot):
        f2_all(slot).wait_recv()
        share_near(slot).start()

    def near_multiply(slot, count=1):
        for i in range(count):
            share_near(slot + i).wait_recv()
        multiply(xn, acc_n, slot, count)

    def far_multiply(slot, count=1):
        for i in range(count):
            share_far(slot + i).wait_recv()
        multiply(xf, acc_f, slot, count)

    def w2_shares(lower, upper):
        for slot in range(lower, upper):
            w2_share(slot).start()

    for slot in range(4):
        w2_share(slot).start()
    pass_on(f1, 1)
    both(1, 3, near_part)
    for slot in range(4, Z):
        w2_share(slot).start()
    pl_all = pl.ds(0, FR)
    remote(far_send.at[pl_all], xf.at[0, 0, pl_all], a1_send, a1_recv, sibling).wait_recv()
    for way, half in parts_of(1):
        a2(1, way, half).start()
    share_far(0).start()
    pass_on(f1, 2)
    both(3, 5, near_part)
    near_in(0)
    pltpu.make_async_copy(w_in.at[0], w1, w1_sem).wait()
    pass_on(a2, 1)
    share_far(1).start()
    share_far(2).start()
    pass_on(f1, 3)
    both(5, 7, near_part)
    both(1, 3, near_in)
    far_multiply(0, 1)
    near_multiply(0, 1)
    pass_on(a2, 2)
    share_far(3).start()
    share_far(4).start()
    pass_on(f1, 4)
    both(7, 8, near_part)

    logit_copy = remote(lg, lg_other, l_send, l_recv, sibling)
    logit_copy.start()
    both(3, 5, near_in)
    far_multiply(1, 2)
    pass_on(a2, 3)
    share_far(5).start()
    share_far(6).start()
    near_multiply(1, 2)
    both(5, 7, near_in)
    far_multiply(3, 2)
    near_multiply(3, 2)
    pass_on(a2, 4)
    share_far(7).start()
    near_in(7)
    far_multiply(5, 2)
    near_multiply(5, 2)
    far_multiply(7, 1)

    def share_hidden(buffer, which):
        return remote(
            buffer.at[:, pl.ds(0, HID)], buffer.at[:, pl.ds(HID, HID)], h_send.at[which], h_recv.at[which], sibling,
        )

    hf[:, 0:HID] = jax.nn.gelu(acc_f[...], approximate=True).astype(BF16)
    share_hidden(hf, 1).start()
    near_multiply(7, 1)
    hn[:, 0:HID] = jax.nn.gelu(acc_n[...], approximate=True).astype(BF16)
    share_hidden(hn, 0).start()
    own_half, other_half = w2.at[:, pl.ds(0, HID)], w2.at[:, pl.ds(HID, HID)]
    pltpu.make_async_copy(own_half, own_half, w2_sem).wait()
    w2_all = remote(own_half, other_half, w2s_send, w2s_recv, sibling)
    w2_all.wait_recv()

    def bn(slot, p):
        block = pl.ds(p * CAP, CAP)
        return remote(
            pn.at[slot, block], rn.at[slot, block], bn_send, bn_recv.at[slot], back[p]
        )

    def bn_all(slot):
        block = pl.ds(0, NR - CAP)
        return remote(
            pn.at[slot, block], rn.at[slot, block], bn_send, bn_recv.at[slot], sibling
        )

    def second(buffer, slot):
        return jnp.dot(buffer[...], w2[slot], preferred_element_type=F32).astype(BF16)

    def near_out(index):
        slot = 7 - index
        terms = second(hn, slot)
        pn[slot] = terms
        rn[slot, SELF * CAP:(SELF + 1) * CAP, :] = terms[SELF * CAP:(SELF + 1) * CAP, :]
        for p in NEAR_ORDER:
            bn(slot, p).start()

    def far_out(index):
        slot = 7 - index
        pf[slot] = second(hf, slot)

    def reduce_copy(own, received, halves, send, recv, step, way, half):
        start, size = halves[half]
        return remote(
            own.at[back_slot(step, way), pl.ds(start, size)], received.at[way, step - 1, pl.ds(start, size)],
            send, recv.at[step - 1, way, half], along[way],
        )

    bf = functools.partial(reduce_copy, pf, rf, F_HALF, bf_send, bf_recv)
    bm = functools.partial(reduce_copy, pm, rm, M_HALF, bm_send, bm_recv)

    def reduce_step(transfer, own, received, halves, step, chosen=None):
        for way, half in chosen or back_parts_of(step):
            if step > 1 and (way, half) in back_parts_of(step - 1):
                transfer(step - 1, way, half).wait_recv()
                start, size = halves[half]
                slot = back_slot(step, way)
                own[slot, start:start + size, :] = (
                    own[slot, start:start + size, :].astype(F32)
                    + received[way, step - 2, start:start + size, :].astype(F32)
                ).astype(BF16)
            transfer(step, way, half).start()

    fresh, held = ((0, 1), (1, 0)), ((0, 0), (1, 1))

    def mix(slot):
        bn_all(slot).wait_recv()
        pm[slot] = jnp.dot(cn[...], rn[slot], preferred_element_type=F32).astype(BF16)

    def mix_down(index):
        mix(7 - index)

    share_hidden(hf, 1).wait_recv()
    both(0, 1, far_out)
    reduce_step(bf, pf, rf, F_HALF, 1)
    both(1, 3, far_out)
    reduce_step(bf, pf, rf, F_HALF, 2, fresh)
    share_hidden(hn, 0).wait_recv()
    both(0, 2, near_out)
    both(2, 3, near_out)
    logit_copy.wait()
    raised = jnp.exp(lg[...] + lg_other[...])
    probs = raised / jnp.sum(raised, axis=0, keepdims=True)
    chosen_first = jnp.sum(jnp.where(names == routing[0:1, :], probs, 0.0), axis=0, keepdims=True)
    chosen_second = jnp.sum(jnp.where(names == routing[1:2, :], probs, 0.0), axis=0, keepdims=True)
    packed = jnp.concatenate(
        [base[0:1, :], base[1:2, :], chosen_first, chosen_second, jnp.zeros((124, GROUP), F32)], axis=0
    )
    packed = jnp.transpose(packed)
    at_first, at_second = packed[:, 0:1].astype(jnp.int32), packed[:, 1:2].astype(jnp.int32)
    by_first, by_second = packed[:, 2:3], packed[:, 3:4]

    def weights(start, size):
        columns = lax.broadcasted_iota(jnp.int32, (GROUP, size), 1) + start
        return (
            jnp.where(columns == at_first, by_first, 0.0) + jnp.where(columns == at_second, by_second, 0.0)
        ).astype(BF16)

    cn[...] = weights(0, NR)
    cf[...] = weights(NR, FR)

    both(3, 4, near_out)
    both(3, 5, far_out)
    reduce_step(bf, pf, rf, F_HALF, 2, held)
    both(4, 5, near_out)
    reduce_step(bf, pf, rf, F_HALF, 3, fresh)
    both(5, 7, far_out)
    both(5, 6, near_out)
    both(0, 1, mix_down)
    reduce_step(bm, pm, rm, M_HALF, 1)
    both(6, 7, near_out)
    reduce_step(bf, pf, rf, F_HALF, 3, held)
    reduce_step(bf, pf, rf, F_HALF, 4, fresh)
    both(1, 2, mix_down)
    reduce_step(bm, pm, rm, M_HALF, 2, fresh[:1])
    both(7, 8, near_out)
    both(2, 3, mix_down)
    reduce_step(bm, pm, rm, M_HALF, 2, fresh[1:])
    both(7, 8, far_out)
    reduce_step(bm, pm, rm, M_HALF, 2, held)
    reduce_step(bf, pf, rf, F_HALF, 4, held)
    both(3, 5, mix_down)
    reduce_step(bm, pm, rm, M_HALF, 3)

    for way, half in back_parts_of(4):
        bf(4, way, half).wait_recv()
    fr[...] = (
        pf[0].astype(F32) + rf[0, 3].astype(F32) + rf[1, 3].astype(F32)
    ).astype(BF16)

    def far_back(p):
        block = pl.ds((p - NEAR) * CAP, CAP)
        return remote(fr.at[block], ra.at[block], ra_send, ra_recv, back[p])

    for p in FAR_ORDER:
        far_back(p).start()
    both(5, 7, mix_down)
    reduce_step(bm, pm, rm, M_HALF, 4)
    both(7, 8, mix_down)
    remote(fr, ra, ra_send, ra_recv, sibling).wait_recv()
    far_term[...] = jnp.dot(cf[...], ra[...], preferred_element_type=F32) + pm[0].astype(F32)
    for way, half in back_parts_of(4):
        bm(4, way, half).wait_recv()
    out[...] = (far_term[...] + rm[0, 3].astype(F32) + rm[1, 3].astype(F32)).astype(BF16)

    def sent(ref, semaphore):
        remote(ref, ref, semaphore, semaphore, sibling).wait_send()

    ring_blocks, most = pl.ds(0, Z - 1), pl.ds(0, NR - CAP)
    sent(tg.at[ring_blocks], f1_send)
    sent(far_send, a1_send)
    sent(near_send.at[:, most], f2_send)
    sent(xf.at[ring_blocks, 0], a2_send)
    sent(xn.at[:, 0], sn_send)
    sent(xf.at[:, 0], sf_send)
    sent(pf.at[ring_blocks], bf_send)
    sent(pm.at[ring_blocks], bm_send)
    sent(pn.at[:, most], bn_send)
    sent(fr, ra_send)
    w2_all.wait_send()
    share_hidden(hn, 0).wait_send()
    share_hidden(hf, 1).wait_send()


def layer(tokens, routing, gate_weight, expert_in, expert_out):
    vmem = pl.BlockSpec(memory_space=pltpu.VMEM)
    anywhere = pl.BlockSpec(memory_space=pl.ANY)
    dma = pltpu.SemaphoreType.DMA
    return pl.pallas_call(
        kernel,
        out_shape=pltpu.VMEM((GROUP, W), BF16),
        in_specs=[anywhere] * 5,
        out_specs=vmem,
        scratch_shapes=[
            pltpu.VMEM((Z, TB, W), BF16),
            pltpu.VMEM((EXPERTS * CAP, GROUP), BF16),
            pltpu.VMEM((Z, NR, W), BF16),
            pltpu.VMEM((FR, W), BF16),
            pltpu.VMEM((Z, 2, NR, W), BF16),
            pltpu.VMEM((Z, 2, FR, W), BF16),
            pltpu.VMEM((NR, HID), F32),
            pltpu.VMEM((FR, HID), F32),
            pltpu.VMEM((Z * 2 * W, HID), BF16),
            pltpu.VMEM((Z, 2 * HID, W), BF16),
            pltpu.VMEM((NR, 2 * HID), BF16),
            pltpu.VMEM((FR, 2 * HID), BF16),
            pltpu.VMEM((Z, FR, W), BF16),
            pltpu.VMEM((2, 4, FR, W), BF16),
            pltpu.VMEM((Z, NR, W), BF16),
            pltpu.VMEM((Z, NR, W), BF16),
            pltpu.VMEM((Z, GROUP, W), BF16),
            pltpu.VMEM((2, 4, GROUP, W), BF16),
            pltpu.VMEM((FR, W), BF16),
            pltpu.VMEM((FR, W), BF16),
            pltpu.VMEM((GROUP, NR), BF16),
            pltpu.VMEM((GROUP, FR), BF16),
            pltpu.VMEM((EXPERTS, GROUP), F32),
            pltpu.VMEM((EXPERTS, GROUP), F32),
            pltpu.VMEM((8, GROUP), F32),
            pltpu.VMEM((GROUP, W), F32),
            pltpu.VMEM((2, GROUP), jnp.int32),
            dma, dma, dma, dma, dma, dma, dma,
            dma, dma((4, 2, 2)), dma, dma, dma, dma((Z,)), dma, dma((4, 2, 2)),
            dma, dma((Z,)), dma, dma((Z,)), dma((2,)), dma((2,)), dma, dma,
            dma, dma((4, 2, 2)), dma, dma((Z,)), dma, dma((4, 2, 2)), dma, dma,
        ],
        compiler_params=pltpu.CompilerParams(collective_id=0, has_side_effects=True),
        name="experts",
    )(tokens, routing.T, gate_weight.T, expert_in, expert_out)


def solution(mesh):
    return jax.shard_map(
        layer,
        mesh=mesh,
        in_specs=(
            P("dp", "expert"),
            P("dp", None),
            P("expert", None),
            P("dp", None, "expert"),
            P("dp", "expert", None),
        ),
        out_specs=P("dp", "expert"),
        check_vma=False,
    )
```

```python
import functools

import jax
import jax.numpy as jnp
from jax import lax
from jax.experimental import pallas as pl
from jax.experimental.pallas import tpu as pltpu
from jax.sharding import PartitionSpec as P

MESH = pl.DeviceIdType.MESH
F32 = jnp.float32
BF16 = jnp.bfloat16

X, Y, Z = 4, 4, 8
GROUP, CAP, EXPERTS, W, HID = 256, 48, 16, 256, 512
SHIFTS = [(dx, dy) for dy in (-1, 0, 1) for dx in (-1, 0, 1)]
SHIFTS += [(2, 0), (0, 2), (2, -1), (2, 1), (2, 2), (-1, 2), (1, 2)]
NEAR, FAR, SELF = 11, 5, 4
NR, FR = NEAR * CAP, FAR * CAP
NEAR_ORDER = [1, 3, 7, 5, 9, 10, 0, 8, 2, 6]
FAR_ORDER = [13, 11, 14, 12, 15]
TB = GROUP + EXPERTS
T_PIECES = ((0, 128), (128, TB - 128))
F_PIECES = ((0, 3 * CAP), (3 * CAP, FR - 3 * CAP))
M_PIECES = ((0, 128), (128, 128))
N_PIECES = ((0, 6 * CAP), (6 * CAP, NR - 6 * CAP))


def far_parts(count):
    half = count // 2
    return [(way, i + half * way) for i in range(half) for way in (0, 1)]


def short_parts(count):
    half = count // 2
    return [(way, i + half * (1 - way)) for i in range(half) for way in (0, 1)]


def parts_of(step, count):
    return far_parts(count) if step == 4 else far_parts(count) + short_parts(count)


def back_parts_of(step, count):
    return far_parts(count) if step == 1 else short_parts(count) + far_parts(count)


def offset_of(slot):
    return 4 if slot == 7 else (slot // 2 if slot % 2 == 0 else -((slot + 1) // 2))


def gather_slots(step, way):
    source = 0 if step == 1 else 2 * step - 3 + way
    return source, (7 if step == 4 else 2 * step - 1 + way)


def back_slot(step, way):
    return 7 if step == 1 else 2 * (5 - step) - way


def kernel(
    tokens, picks, gate, w_in, w_out, out,
    tg, assign, near_send, far_send, xn, xf, acc_n, acc_f, w1, w2, hn, hf,
    pf, rf, pn, rn, pm, rm, fr, ra, cn, cf, lg, lg_other, base, far_term, routing,
    tok_sem, gate_sem, picks_sem, w1_sem, w2_sem, w2s_send, w2s_recv,
    f1_send, f1_recv, a1_send, a1_recv, f2_send, f2_recv, a2_send, a2_recv,
    sn_send, sn_recv, sf_send, sf_recv, h_send, h_recv, l_send, l_recv,
    bf_send, bf_recv, bn_send, bn_recv, bm_send, bm_recv, ra_send, ra_recv,
):
    dp = lax.axis_index("dp")
    ex = lax.axis_index("expert")
    gy, gx = lax.div(dp, X), lax.rem(dp, X)
    z, core = lax.div(ex, 2), lax.rem(ex, 2)

    def plane(dx, dy):
        return (lax.rem(gy + dy + Y, Y) * X + lax.rem(gx + dx + X, X), ex)

    def ring(offset):
        return lax.rem(z + offset + Z, Z)

    to = [plane(dx, dy) for dx, dy in SHIFTS]
    back = [plane(-dx, -dy) for dx, dy in SHIFTS]
    along = ((dp, ring(1) * 2 + 1 - core), (dp, ring(-1) * 2 + 1 - core))
    sibling = (dp, z * 2 + 1 - core)

    def remote(src, dst, send, recv, device):
        return pltpu.make_async_remote_copy(
            src_ref=src, dst_ref=dst, send_sem=send, recv_sem=recv,
            device_id=device, device_id_type=MESH,
        )

    barrier = pltpu.get_barrier_semaphore()
    for device in [to[p] for p in range(EXPERTS) if p != SELF] + [*along, sibling]:
        pl.semaphore_signal(barrier, inc=1, device_id=device, device_id_type=MESH)

    picks_copy = pltpu.make_async_copy(picks, routing, picks_sem)
    picks_copy.start()
    token_copy = pltpu.make_async_copy(tokens, tg.at[0, pl.ds(0, GROUP)], tok_sem)
    token_copy.start()
    gate_copy = pltpu.make_async_copy(gate, tg.at[0, pl.ds(GROUP, EXPERTS)], gate_sem)
    gate_copy.start()
    picks_copy.wait()

    def block_of(slot, side):
        offset = offset_of(slot)
        return ring(offset) * 2 + (core if (offset + side) % 2 == 0 else 1 - core)

    def w1_copy(slot, side):
        rows = block_of(slot, side) * W
        return pltpu.make_async_copy(
            w_in.at[0, pl.ds(pl.multiple_of(rows, W), W), :], w1.at[pl.ds((slot * 2 + side) * W, W)], w1_sem
        )

    def w2_columns(slot, side):
        columns = block_of(slot, side) * W
        return w_out.at[0, :, pl.ds(pl.multiple_of(columns, W), W)]

    def w2_copy(slot):
        return pltpu.make_async_copy(w2_columns(slot, 0), w2.at[slot, pl.ds(0, HID)], w2_sem)

    def w2_share(slot):
        return remote(
            w2_columns(slot, 1), w2.at[slot, pl.ds(HID, HID)], w2s_send, w2s_recv, sibling
        )

    def f1(step, way, half):
        source, target = gather_slots(step, way)
        start, size = T_PIECES[half]
        return remote(
            tg.at[source, pl.ds(start, size)], tg.at[target, pl.ds(start, size)],
            f1_send, f1_recv.at[step - 1, way, half], along[way],
        )

    def a1(p):
        block = pl.ds((p - NEAR) * CAP, CAP)
        return remote(far_send.at[block], xf.at[0, 0, block], a1_send, a1_recv, to[p])

    def f2(slot, p):
        block = pl.ds(p * CAP, CAP)
        return remote(
            near_send.at[slot, block], xn.at[slot, 0, block], f2_send, f2_recv.at[slot], to[p]
        )

    def f2_all(slot):
        block = pl.ds(0, NR - CAP)
        return remote(
            near_send.at[slot, block], xn.at[slot, 0, block], f2_send, f2_recv.at[slot], sibling
        )

    def a2(step, way, half):
        source, target = gather_slots(step, way)
        start, size = F_PIECES[half]
        return remote(
            xf.at[source, 0, pl.ds(start, size)], xf.at[target, 0, pl.ds(start, size)],
            a2_send, a2_recv.at[step - 1, way, half], along[way],
        )

    def share_near(slot):
        return remote(xn.at[slot, 0], xn.at[slot, 1], sn_send, sn_recv.at[slot], sibling)

    def share_far(slot):
        return remote(xf.at[slot, 0], xf.at[slot, 1], sf_send, sf_recv.at[slot], sibling)

    def send_near(slot):
        for p in NEAR_ORDER:
            f2(slot, p).start()

    def pass_on(transfer, step, chosen=None):
        for way, half in chosen or parts_of(step, 2):
            transfer(step, way, half).wait_recv()
            if step < 4 and (way, half) in parts_of(step + 1, 2):
                transfer(step + 1, way, half).start()

    names = lax.broadcasted_iota(jnp.int32, (EXPERTS, GROUP), 0)
    sx = (lax.rem(names, X) - gx + 1 + X) & 3
    sy = (lax.div(names, X) - gy + 1 + Y) & 3
    place = sy * 3 + sx
    for p in range(9, EXPERTS):
        dx, dy = SHIFTS[p]
        place = jnp.where((sx == dx + 1) & (sy == dy + 1), p, place)
    place = (place * CAP).astype(F32)
    first = (names == routing[0:1, :]).astype(F32)
    second = (names == routing[1:2, :]).astype(F32)
    earlier = lax.broadcasted_iota(jnp.int32, (GROUP, GROUP), 0)
    later = lax.broadcasted_iota(jnp.int32, (GROUP, GROUP), 1)
    upper = (earlier < later).astype(F32).astype(BF16)
    before_first = jnp.dot(first.astype(BF16), upper, preferred_element_type=F32)
    before_second = jnp.dot(second.astype(BF16), upper, preferred_element_type=F32)
    before_second = before_second + jnp.sum(first, axis=1, keepdims=True)
    row_first = jnp.sum(first * (place + before_first), axis=0, keepdims=True)
    row_second = jnp.sum(second * (place + before_second), axis=0, keepdims=True)
    rows = lax.broadcasted_iota(jnp.int32, (EXPERTS * CAP, GROUP), 0)
    hit = (rows == row_first.astype(jnp.int32)) | (rows == row_second.astype(jnp.int32))
    assign[...] = hit.astype(F32).astype(BF16)
    base[0:1, :] = row_first
    base[1:2, :] = row_second
    lg[...] = jnp.zeros_like(lg)

    token_copy.wait()
    gate_copy.wait()
    pl.semaphore_wait(barrier, 18)
    for way, half in parts_of(1, 2):
        f1(1, way, half).start()
    far_send[...] = jnp.dot(
        assign[NR:, :], tg[0, 0:GROUP, :], preferred_element_type=F32
    ).astype(BF16)

    def dispatch_near(slot):
        rows_of = jnp.dot(assign[0:NR, :], tg[slot, 0:GROUP, :], preferred_element_type=F32).astype(BF16)
        near_send[slot] = rows_of
        xn[slot, 0, SELF * CAP:(SELF + 1) * CAP, :] = rows_of[SELF * CAP:(SELF + 1) * CAP, :]
        lg[...] += lax.dot_general(
            tg[slot, GROUP:TB, :], tg[slot, 0:GROUP, :], (((1,), (1,)), ((), ())), preferred_element_type=F32
        )

    for p in FAR_ORDER:
        a1(p).start()
    dispatch_near(0)
    send_near(0)
    for slot in range(Z):
        for side in range(2):
            w1_copy(slot, side).start()
    for slot in range(Z):
        w2_copy(slot).start()

    acc_n[...] = jnp.zeros_like(acc_n)
    acc_f[...] = jnp.zeros_like(acc_f)

    def both(lower, upper, work):
        lax.fori_loop(lower, upper, lambda slot, carry: (work(slot), carry)[1], 0)

    def near_part(slot):
        dispatch_near(slot)
        send_near(slot)

    def multiply(rows_of, total, slot, count):
        columns = [rows_of[slot + i, side] for i in range(count) for side in range(2)]
        depth = 2 * W * count
        start = pl.multiple_of(slot * 2 * W, 2 * W)
        total[...] += jnp.dot(
            jnp.concatenate(columns, axis=1), w1[pl.ds(start, depth), :], preferred_element_type=F32
        )

    def near_in(slot):
        f2_all(slot).wait_recv()
        share_near(slot).start()

    def near_multiply(slot, count=1):
        for i in range(count):
            share_near(slot + i).wait_recv()
        multiply(xn, acc_n, slot, count)

    def far_multiply(slot, count=1):
        for i in range(count):
            share_far(slot + i).wait_recv()
        multiply(xf, acc_f, slot, count)

    def w2_shares(lower, upper):
        for slot in range(lower, upper):
            w2_share(slot).start()

    for slot in range(4):
        w2_share(slot).start()
    pass_on(f1, 1)
    both(1, 3, near_part)
    for slot in range(4, Z):
        w2_share(slot).start()
    pl_all = pl.ds(0, FR)
    remote(far_send.at[pl_all], xf.at[0, 0, pl_all], a1_send, a1_recv, sibling).wait_recv()
    for way, half in far_parts(2):
        a2(1, way, half).start()
    share_far(0).start()
    pass_on(f1, 2)
    for way, half in short_parts(2):
        a2(1, way, half).start()
    both(3, 5, near_part)
    near_in(0)
    pltpu.make_async_copy(w_in.at[0], w1, w1_sem).wait()
    pass_on(a2, 1, far_parts(2))
    near_multiply(0, 1)
    far_multiply(0, 1)
    pass_on(f1, 3)
    both(5, 7, near_part)
    both(1, 3, near_in)
    pass_on(a2, 1, short_parts(2))
    share_far(1).start()
    share_far(2).start()
    pass_on(a2, 2, far_parts(2))
    pass_on(f1, 4)
    both(7, 8, near_part)

    logit_copy = remote(lg, lg_other, l_send, l_recv, sibling)
    logit_copy.start()
    both(3, 5, near_in)
    pass_on(a2, 2, short_parts(2))
    share_far(3).start()
    share_far(4).start()
    near_multiply(1, 2)
    far_multiply(1, 2)
    pass_on(a2, 3, far_parts(2))
    both(5, 7, near_in)
    near_multiply(3, 2)
    far_multiply(3, 2)
    pass_on(a2, 3, short_parts(2))
    share_far(5).start()
    share_far(6).start()
    near_in(7)
    near_multiply(5, 2)
    pass_on(a2, 4)
    share_far(7).start()
    far_multiply(5, 2)

    def share_hidden(buffer, start, size, which):
        rows = pl.ds(start, size)
        return remote(
            buffer.at[rows, pl.ds(0, HID)], buffer.at[rows, pl.ds(HID, HID)],
            h_send.at[which], h_recv.at[which], sibling,
        )

    near_shares = [share_hidden(hn, start, size, which) for which, (start, size) in enumerate(N_PIECES)]
    far_share = share_hidden(hf, 0, FR, 2)
    share_near(7).wait_recv()
    for share, (start, size) in zip(near_shares, N_PIECES):
        stop = start + size
        total = acc_n[start:stop, :] + jnp.dot(
            jnp.concatenate([xn[7, 0, start:stop, :], xn[7, 1, start:stop, :]], axis=1),
            w1[14 * W:16 * W, :], preferred_element_type=F32,
        )
        hn[start:stop, 0:HID] = jax.nn.gelu(total, approximate=True).astype(BF16)
        share.start()
    far_multiply(7, 1)
    hf[:, 0:HID] = jax.nn.gelu(acc_f[...], approximate=True).astype(BF16)
    far_share.start()
    own_half, other_half = w2.at[:, pl.ds(0, HID)], w2.at[:, pl.ds(HID, HID)]
    pltpu.make_async_copy(own_half, own_half, w2_sem).wait()
    w2_all = remote(own_half, other_half, w2s_send, w2s_recv, sibling)
    w2_all.wait_recv()

    def bn(slot, p):
        block = pl.ds(p * CAP, CAP)
        return remote(
            pn.at[slot, block], rn.at[slot, block], bn_send, bn_recv.at[slot], back[p]
        )

    def bn_all(slot):
        block = pl.ds(0, NR - CAP)
        return remote(
            pn.at[slot, block], rn.at[slot, block], bn_send, bn_recv.at[slot], sibling
        )

    def second(buffer, slot):
        return jnp.dot(buffer[...], w2[slot], preferred_element_type=F32).astype(BF16)

    def near_out(index):
        slot = 7 - index
        terms = second(hn, slot)
        pn[slot] = terms
        rn[slot, SELF * CAP:(SELF + 1) * CAP, :] = terms[SELF * CAP:(SELF + 1) * CAP, :]
        for p in NEAR_ORDER:
            bn(slot, p).start()

    def far_out(index):
        slot = 7 - index
        pf[slot] = second(hf, slot)

    def reduce_copy(own, received, halves, send, recv, step, way, half):
        start, size = halves[half]
        return remote(
            own.at[back_slot(step, way), pl.ds(start, size)], received.at[way, step - 1, pl.ds(start, size)],
            send, recv.at[step - 1, way, half], along[way],
        )

    bf = functools.partial(reduce_copy, pf, rf, F_PIECES, bf_send, bf_recv)
    bm = functools.partial(reduce_copy, pm, rm, M_PIECES, bm_send, bm_recv)

    def reduce_step(transfer, own, received, halves, step, chosen=None):
        count = len(halves)
        for way, half in chosen or back_parts_of(step, count):
            if step > 1 and (way, half) in back_parts_of(step - 1, count):
                transfer(step - 1, way, half).wait_recv()
                start, size = halves[half]
                slot = back_slot(step, way)
                own[slot, start:start + size, :] = (
                    own[slot, start:start + size, :].astype(F32)
                    + received[way, step - 2, start:start + size, :].astype(F32)
                ).astype(BF16)
            transfer(step, way, half).start()

    fresh, held = short_parts(2), far_parts(2)

    def one_way(parts, which):
        return [(way, half) for way, half in parts if way == which]


    def mix(slot):
        bn_all(slot).wait_recv()
        pm[slot] = jnp.dot(cn[...], rn[slot], preferred_element_type=F32).astype(BF16)

    def mix_down(index):
        mix(7 - index)

    for share in near_shares:
        share.wait_recv()
    both(0, 1, near_out)
    far_share.wait_recv()
    both(0, 1, far_out)
    reduce_step(bf, pf, rf, F_PIECES, 1)
    both(1, 3, far_out)
    reduce_step(bf, pf, rf, F_PIECES, 2, fresh)
    both(1, 3, near_out)
    logit_copy.wait()
    raised = jnp.exp(lg[...] + lg_other[...])
    probs = raised / jnp.sum(raised, axis=0, keepdims=True)
    chosen_first = jnp.sum(jnp.where(names == routing[0:1, :], probs, 0.0), axis=0, keepdims=True)
    chosen_second = jnp.sum(jnp.where(names == routing[1:2, :], probs, 0.0), axis=0, keepdims=True)
    packed = jnp.concatenate(
        [base[0:1, :], base[1:2, :], chosen_first, chosen_second, jnp.zeros((124, GROUP), F32)], axis=0
    )
    packed = jnp.transpose(packed)
    at_first, at_second = packed[:, 0:1].astype(jnp.int32), packed[:, 1:2].astype(jnp.int32)
    by_first, by_second = packed[:, 2:3], packed[:, 3:4]

    def weights(start, size):
        columns = lax.broadcasted_iota(jnp.int32, (GROUP, size), 1) + start
        return (
            jnp.where(columns == at_first, by_first, 0.0) + jnp.where(columns == at_second, by_second, 0.0)
        ).astype(BF16)

    cn[...] = weights(0, NR)
    cf[...] = weights(NR, FR)

    both(3, 5, far_out)
    reduce_step(bf, pf, rf, F_PIECES, 2, held)
    both(3, 4, near_out)
    reduce_step(bf, pf, rf, F_PIECES, 3, fresh)
    both(0, 1, mix_down)
    reduce_step(bm, pm, rm, M_PIECES, 1)
    both(5, 7, far_out)
    both(4, 5, near_out)
    both(1, 2, mix_down)
    reduce_step(bm, pm, rm, M_PIECES, 2, one_way(fresh, 0))
    reduce_step(bf, pf, rf, F_PIECES, 3, held)
    both(5, 6, near_out)
    reduce_step(bf, pf, rf, F_PIECES, 4, fresh)
    both(2, 3, mix_down)
    reduce_step(bm, pm, rm, M_PIECES, 2, one_way(fresh, 1))
    reduce_step(bm, pm, rm, M_PIECES, 2, held)
    both(6, 7, near_out)
    both(7, 8, far_out)
    both(3, 4, mix_down)
    reduce_step(bf, pf, rf, F_PIECES, 4, held)
    both(7, 8, near_out)
    both(4, 5, mix_down)
    reduce_step(bm, pm, rm, M_PIECES, 3)

    for way, half in back_parts_of(4, 2):
        bf(4, way, half).wait_recv()
    fr[...] = (
        pf[0].astype(F32) + rf[0, 3].astype(F32) + rf[1, 3].astype(F32)
    ).astype(BF16)

    def far_back(p):
        block = pl.ds((p - NEAR) * CAP, CAP)
        return remote(fr.at[block], ra.at[block], ra_send, ra_recv, back[p])

    for p in FAR_ORDER:
        far_back(p).start()
    both(5, 7, mix_down)
    reduce_step(bm, pm, rm, M_PIECES, 4)
    both(7, 8, mix_down)
    remote(fr, ra, ra_send, ra_recv, sibling).wait_recv()
    far_term[...] = jnp.dot(cf[...], ra[...], preferred_element_type=F32) + pm[0].astype(F32)
    for way, half in back_parts_of(4, 2):
        bm(4, way, half).wait_recv()
    out[...] = (far_term[...] + rm[0, 3].astype(F32) + rm[1, 3].astype(F32)).astype(BF16)

    def sent(ref, semaphore):
        remote(ref, ref, semaphore, semaphore, sibling).wait_send()

    ring_blocks, most = pl.ds(0, Z - 1), pl.ds(0, NR - CAP)
    sent(tg.at[ring_blocks], f1_send)
    sent(far_send, a1_send)
    sent(near_send.at[:, most], f2_send)
    sent(xf.at[ring_blocks, 0], a2_send)
    sent(xn.at[:, 0], sn_send)
    sent(xf.at[:, 0], sf_send)
    sent(pf.at[ring_blocks], bf_send)
    sent(pm.at[ring_blocks], bm_send)
    sent(pn.at[:, most], bn_send)
    sent(fr, ra_send)
    w2_all.wait_send()
    for share in [*near_shares, far_share]:
        share.wait_send()


def layer(tokens, routing, gate_weight, expert_in, expert_out):
    vmem = pl.BlockSpec(memory_space=pltpu.VMEM)
    anywhere = pl.BlockSpec(memory_space=pl.ANY)
    dma = pltpu.SemaphoreType.DMA
    return pl.pallas_call(
        kernel,
        out_shape=pltpu.VMEM((GROUP, W), BF16),
        in_specs=[anywhere] * 5,
        out_specs=vmem,
        scratch_shapes=[
            pltpu.VMEM((Z, TB, W), BF16),
            pltpu.VMEM((EXPERTS * CAP, GROUP), BF16),
            pltpu.VMEM((Z, NR, W), BF16),
            pltpu.VMEM((FR, W), BF16),
            pltpu.VMEM((Z, 2, NR, W), BF16),
            pltpu.VMEM((Z, 2, FR, W), BF16),
            pltpu.VMEM((NR, HID), F32),
            pltpu.VMEM((FR, HID), F32),
            pltpu.VMEM((Z * 2 * W, HID), BF16),
            pltpu.VMEM((Z, 2 * HID, W), BF16),
            pltpu.VMEM((NR, 2 * HID), BF16),
            pltpu.VMEM((FR, 2 * HID), BF16),
            pltpu.VMEM((Z, FR, W), BF16),
            pltpu.VMEM((2, 4, FR, W), BF16),
            pltpu.VMEM((Z, NR, W), BF16),
            pltpu.VMEM((Z, NR, W), BF16),
            pltpu.VMEM((Z, GROUP, W), BF16),
            pltpu.VMEM((2, 4, GROUP, W), BF16),
            pltpu.VMEM((FR, W), BF16),
            pltpu.VMEM((FR, W), BF16),
            pltpu.VMEM((GROUP, NR), BF16),
            pltpu.VMEM((GROUP, FR), BF16),
            pltpu.VMEM((EXPERTS, GROUP), F32),
            pltpu.VMEM((EXPERTS, GROUP), F32),
            pltpu.VMEM((8, GROUP), F32),
            pltpu.VMEM((GROUP, W), F32),
            pltpu.VMEM((2, GROUP), jnp.int32),
            dma, dma, dma, dma, dma, dma, dma,
            dma, dma((4, 2, 2)), dma, dma, dma, dma((Z,)), dma, dma((4, 2, 2)),
            dma, dma((Z,)), dma, dma((Z,)), dma((3,)), dma((3,)), dma, dma,
            dma, dma((4, 2, 2)), dma, dma((Z,)), dma, dma((4, 2, 2)), dma, dma,
        ],
        compiler_params=pltpu.CompilerParams(collective_id=0, has_side_effects=True),
        name="experts",
    )(tokens, routing.T, gate_weight.T, expert_in, expert_out)


def solution(mesh):
    return jax.shard_map(
        layer,
        mesh=mesh,
        in_specs=(
            P("dp", "expert"),
            P("dp", None),
            P("expert", None),
            P("dp", None, "expert"),
            P("dp", "expert", None),
        ),
        out_specs=P("dp", "expert"),
        check_vma=False,
    )
```

```python
import functools

import jax
import jax.numpy as jnp
from jax import lax
from jax.experimental import pallas as pl
from jax.experimental.pallas import tpu as pltpu
from jax.sharding import PartitionSpec as P

MESH = pl.DeviceIdType.MESH
F32 = jnp.float32
BF16 = jnp.bfloat16

X, Y, Z = 4, 4, 8
GROUP, CAP, EXPERTS, W, HID = 256, 48, 16, 256, 512
SHIFTS = [(dx, dy) for dy in (-1, 0, 1) for dx in (-1, 0, 1)]
SHIFTS += [(2, 0), (0, 2), (2, -1), (2, 1), (2, 2), (-1, 2), (1, 2)]
NEAR, FAR, SELF = 11, 5, 4
NR, FR = NEAR * CAP, FAR * CAP
NEAR_ORDER = [0, 8, 9, 10, 2, 6, 1, 3, 7, 5]
FAR_ORDER = [13, 11, 14, 12, 15]
TB = GROUP + EXPERTS
T_PIECES = ((0, 128), (128, TB - 128))
F_PIECES = ((0, 3 * CAP), (3 * CAP, FR - 3 * CAP))
M_PIECES = ((0, 64), (64, 64), (128, 64), (192, 64))
N_PIECES = ((0, 6 * CAP), (6 * CAP, NR - 6 * CAP))


def far_parts(count):
    half = count // 2
    return [(way, i + half * way) for i in range(half) for way in (0, 1)]


def short_parts(count):
    half = count // 2
    return [(way, i + half * (1 - way)) for i in range(half) for way in (0, 1)]


def parts_of(step, count):
    return far_parts(count) if step == 4 else far_parts(count) + short_parts(count)


def back_parts_of(step, count):
    return far_parts(count) if step == 1 else short_parts(count) + far_parts(count)


def offset_of(slot):
    return 4 if slot == 7 else (slot // 2 if slot % 2 == 0 else -((slot + 1) // 2))


def gather_slots(step, way):
    source = 0 if step == 1 else 2 * step - 3 + way
    return source, (7 if step == 4 else 2 * step - 1 + way)


def back_slot(step, way):
    return 7 if step == 1 else 2 * (5 - step) - way


def kernel(
    tokens, picks, gate, w_in, w_out, out,
    tg, assign, near_send, far_send, xn, xf, acc_n, acc_f, w1, w2, hn, hf,
    pf, rf, pn, rn, pm, rm, fr, ra, cn, cf, lg, lg_other, base, far_term, routing, first_near, first_far,
    tok_sem, gate_sem, picks_sem, w1_sem, w2_sem, w2s_send, w2s_recv,
    f1_send, f1_recv, a1_send, a1_recv, f2_send, f2_recv, a2_send, a2_recv,
    sn_send, sn_recv, sf_send, sf_recv, h_send, h_recv, l_send, l_recv,
    bf_send, bf_recv, bn_send, bn_recv, bm_send, bm_recv, ra_send, ra_recv,
):
    dp = lax.axis_index("dp")
    ex = lax.axis_index("expert")
    gy, gx = lax.div(dp, X), lax.rem(dp, X)
    z, core = lax.div(ex, 2), lax.rem(ex, 2)

    def plane(dx, dy):
        return (lax.rem(gy + dy + Y, Y) * X + lax.rem(gx + dx + X, X), ex)

    def ring(offset):
        return lax.rem(z + offset + Z, Z)

    to = [plane(dx, dy) for dx, dy in SHIFTS]
    back = [plane(-dx, -dy) for dx, dy in SHIFTS]
    along = ((dp, ring(1) * 2 + 1 - core), (dp, ring(-1) * 2 + 1 - core))
    sibling = (dp, z * 2 + 1 - core)

    def remote(src, dst, send, recv, device):
        return pltpu.make_async_remote_copy(
            src_ref=src, dst_ref=dst, send_sem=send, recv_sem=recv,
            device_id=device, device_id_type=MESH,
        )

    barrier = pltpu.get_barrier_semaphore()
    for device in [to[p] for p in range(EXPERTS) if p != SELF] + [*along, sibling]:
        pl.semaphore_signal(barrier, inc=1, device_id=device, device_id_type=MESH)

    picks_copy = pltpu.make_async_copy(picks, routing, picks_sem)
    picks_copy.start()
    token_copy = pltpu.make_async_copy(tokens, tg.at[0, pl.ds(0, GROUP)], tok_sem)
    token_copy.start()
    gate_copy = pltpu.make_async_copy(gate, tg.at[0, pl.ds(GROUP, EXPERTS)], gate_sem)
    gate_copy.start()
    picks_copy.wait()

    def block_of(slot, side):
        offset = offset_of(slot)
        return ring(offset) * 2 + (core if (offset + side) % 2 == 0 else 1 - core)

    def w1_copy(slot, side):
        rows = block_of(slot, side) * W
        return pltpu.make_async_copy(
            w_in.at[0, pl.ds(pl.multiple_of(rows, W), W), :], w1.at[pl.ds((slot * 2 + side) * W, W)], w1_sem
        )

    def w2_columns(slot, side):
        columns = block_of(slot, side) * W
        return w_out.at[0, :, pl.ds(pl.multiple_of(columns, W), W)]

    def w2_copy(slot):
        return pltpu.make_async_copy(w2_columns(slot, 0), w2.at[slot, pl.ds(0, HID)], w2_sem)

    def w2_share(slot):
        return remote(
            w2_columns(slot, 1), w2.at[slot, pl.ds(HID, HID)], w2s_send, w2s_recv, sibling
        )

    def f1(step, way, half):
        source, target = gather_slots(step, way)
        start, size = T_PIECES[half]
        return remote(
            tg.at[source, pl.ds(start, size)], tg.at[target, pl.ds(start, size)],
            f1_send, f1_recv.at[step - 1, way, half], along[way],
        )

    def a1(p):
        block = pl.ds((p - NEAR) * CAP, CAP)
        return remote(far_send.at[block], xf.at[0, 0, block], a1_send, a1_recv, to[p])

    def f2(slot, p):
        block = pl.ds(p * CAP, CAP)
        return remote(
            near_send.at[slot, block], xn.at[slot, 0, block], f2_send, f2_recv.at[slot], to[p]
        )

    def f2_all(slot):
        block = pl.ds(0, NR - CAP)
        return remote(
            near_send.at[slot, block], xn.at[slot, 0, block], f2_send, f2_recv.at[slot], sibling
        )

    def a2(step, way, half):
        source, target = gather_slots(step, way)
        start, size = F_PIECES[half]
        return remote(
            xf.at[source, 0, pl.ds(start, size)], xf.at[target, 0, pl.ds(start, size)],
            a2_send, a2_recv.at[step - 1, way, half], along[way],
        )

    def share_near(slot):
        return remote(xn.at[slot, 0], xn.at[slot, 1], sn_send, sn_recv.at[slot], sibling)

    def share_far(slot):
        return remote(xf.at[slot, 0], xf.at[slot, 1], sf_send, sf_recv.at[slot], sibling)

    def send_near(slot):
        for p in NEAR_ORDER:
            f2(slot, p).start()

    def pass_on(transfer, step, chosen=None):
        for way, half in chosen or parts_of(step, 2):
            transfer(step, way, half).wait_recv()
            if step < 4 and (way, half) in parts_of(step + 1, 2):
                transfer(step + 1, way, half).start()

    names = lax.broadcasted_iota(jnp.int32, (EXPERTS, GROUP), 0)
    sx = (lax.rem(names, X) - gx + 1 + X) & 3
    sy = (lax.div(names, X) - gy + 1 + Y) & 3
    place = sy * 3 + sx
    for p in range(9, EXPERTS):
        dx, dy = SHIFTS[p]
        place = jnp.where((sx == dx + 1) & (sy == dy + 1), p, place)
    place = (place * CAP).astype(F32)
    first = (names == routing[0:1, :]).astype(F32)
    second = (names == routing[1:2, :]).astype(F32)
    earlier = lax.broadcasted_iota(jnp.int32, (GROUP, GROUP), 0)
    later = lax.broadcasted_iota(jnp.int32, (GROUP, GROUP), 1)
    upper = (earlier < later).astype(F32).astype(BF16)
    before_first = jnp.dot(first.astype(BF16), upper, preferred_element_type=F32)
    before_second = jnp.dot(second.astype(BF16), upper, preferred_element_type=F32)
    before_second = before_second + jnp.sum(first, axis=1, keepdims=True)
    row_first = jnp.sum(first * (place + before_first), axis=0, keepdims=True)
    row_second = jnp.sum(second * (place + before_second), axis=0, keepdims=True)
    rows = lax.broadcasted_iota(jnp.int32, (EXPERTS * CAP, GROUP), 0)
    hit = (rows == row_first.astype(jnp.int32)) | (rows == row_second.astype(jnp.int32))
    assign[...] = hit.astype(F32).astype(BF16)
    base[0:1, :] = row_first
    base[1:2, :] = row_second
    lg[...] = jnp.zeros_like(lg)

    token_copy.wait()
    gate_copy.wait()
    pl.semaphore_wait(barrier, 18)
    for way, half in parts_of(1, 2):
        f1(1, way, half).start()
    far_send[...] = jnp.dot(
        assign[NR:, :], tg[0, 0:GROUP, :], preferred_element_type=F32
    ).astype(BF16)

    def dispatch_near(slot):
        rows_of = jnp.dot(assign[0:NR, :], tg[slot, 0:GROUP, :], preferred_element_type=F32).astype(BF16)
        near_send[slot] = rows_of
        xn[slot, 0, SELF * CAP:(SELF + 1) * CAP, :] = rows_of[SELF * CAP:(SELF + 1) * CAP, :]
        lg[...] += lax.dot_general(
            tg[slot, GROUP:TB, :], tg[slot, 0:GROUP, :], (((1,), (1,)), ((), ())), preferred_element_type=F32
        )

    for p in FAR_ORDER:
        a1(p).start()
    dispatch_near(0)
    send_near(0)
    for slot in range(Z):
        for side in range(2):
            w1_copy(slot, side).start()
    for slot in range(Z):
        w2_copy(slot).start()

    acc_n[...] = jnp.zeros_like(acc_n)
    acc_f[...] = jnp.zeros_like(acc_f)

    none = lax.div(dp, X * Y)

    def both(lower, upper, work):
        lax.fori_loop(lower + none, upper + none, lambda slot, carry: (work(slot), carry)[1], 0)

    def near_part(slot):
        dispatch_near(slot)
        send_near(slot)

    def multiply(rows_of, total, slot, count):
        columns = [rows_of[slot + i, side] for i in range(count) for side in range(2)]
        depth = 2 * W * count
        start = pl.multiple_of(slot * 2 * W, 2 * W)
        total[...] += jnp.dot(
            jnp.concatenate(columns, axis=1), w1[pl.ds(start, depth), :], preferred_element_type=F32
        )

    def near_in(slot):
        f2_all(slot).wait_recv()
        share_near(slot).start()

    def near_multiply(slot, count=1):
        for i in range(count):
            share_near(slot + i).wait_recv()
        multiply(xn, acc_n, slot, count)

    def far_multiply(slot, count=1):
        for i in range(count):
            share_far(slot + i).wait_recv()
        multiply(xf, acc_f, slot, count)

    def w2_shares(lower, upper):
        for slot in range(lower, upper):
            w2_share(slot).start()

    for slot in range(4):
        w2_share(slot).start()
    pass_on(f1, 1)
    both(1, 3, near_part)
    for slot in range(4, Z):
        w2_share(slot).start()
    pl_all = pl.ds(0, FR)
    remote(far_send.at[pl_all], xf.at[0, 0, pl_all], a1_send, a1_recv, sibling).wait_recv()
    for way, half in far_parts(2):
        a2(1, way, half).start()
    share_far(0).start()
    pass_on(f1, 2)
    for way, half in short_parts(2):
        a2(1, way, half).start()
    both(3, 5, near_part)
    near_in(0)
    pltpu.make_async_copy(w_in.at[0], w1, w1_sem).wait()
    pass_on(a2, 1, far_parts(2))
    near_multiply(0, 1)
    far_multiply(0, 1)
    pass_on(f1, 3)
    both(5, 7, near_part)
    both(1, 3, near_in)
    pass_on(a2, 1, short_parts(2))
    share_far(1).start()
    share_far(2).start()
    pass_on(a2, 2, far_parts(2))
    pass_on(f1, 4)
    both(7, 8, near_part)

    logit_copy = remote(lg, lg_other, l_send, l_recv, sibling)
    logit_copy.start()
    both(3, 5, near_in)
    pass_on(a2, 2, short_parts(2))
    share_far(3).start()
    share_far(4).start()
    near_multiply(1, 2)
    far_multiply(1, 2)
    pass_on(a2, 3, far_parts(2))
    both(5, 7, near_in)
    near_multiply(3, 2)
    far_multiply(3, 2)
    pass_on(a2, 3, short_parts(2))
    share_far(5).start()
    share_far(6).start()
    near_in(7)
    near_multiply(5, 2)
    pass_on(a2, 4)
    share_far(7).start()
    far_multiply(5, 2)

    def share_hidden(buffer, start, size, which):
        rows = pl.ds(start, size)
        return remote(
            buffer.at[rows, pl.ds(0, HID)], buffer.at[rows, pl.ds(HID, HID)],
            h_send.at[which], h_recv.at[which], sibling,
        )

    near_shares = [share_hidden(hn, start, size, which) for which, (start, size) in enumerate(N_PIECES)]
    far_share = share_hidden(hf, 0, FR, 2)
    share_near(7).wait_recv()
    for share, (start, size) in zip(near_shares, N_PIECES):
        stop = start + size
        total = acc_n[start:stop, :] + jnp.dot(
            jnp.concatenate([xn[7, 0, start:stop, :], xn[7, 1, start:stop, :]], axis=1),
            w1[14 * W:16 * W, :], preferred_element_type=F32,
        )
        hn[start:stop, 0:HID] = jax.nn.gelu(total, approximate=True).astype(BF16)
        share.start()
    far_multiply(7, 1)
    hf[:, 0:HID] = jax.nn.gelu(acc_f[...], approximate=True).astype(BF16)
    far_share.start()
    own_half, other_half = w2.at[:, pl.ds(0, HID)], w2.at[:, pl.ds(HID, HID)]
    pltpu.make_async_copy(own_half, own_half, w2_sem).wait()
    w2_all = remote(own_half, other_half, w2s_send, w2s_recv, sibling)
    w2_all.wait_recv()

    def bn(slot, p):
        block = pl.ds(p * CAP, CAP)
        return remote(
            pn.at[slot, block], rn.at[slot, block], bn_send, bn_recv.at[slot], back[p]
        )

    def bn_all(slot):
        block = pl.ds(0, NR - CAP)
        return remote(
            pn.at[slot, block], rn.at[slot, block], bn_send, bn_recv.at[slot], sibling
        )

    def second(buffer, slot):
        return jnp.dot(buffer[...], w2[slot], preferred_element_type=F32).astype(BF16)

    def near_out(index):
        slot = 7 - index
        send_back(slot, second(hn, slot))

    def send_back(slot, terms):
        pn[slot] = terms
        rn[slot, SELF * CAP:(SELF + 1) * CAP, :] = terms[SELF * CAP:(SELF + 1) * CAP, :]
        for p in NEAR_ORDER:
            bn(slot, p).start()

    def far_out(index):
        slot = 7 - index
        pf[slot] = second(hf, slot)

    def reduce_copy(own, received, halves, send, recv, step, way, half):
        start, size = halves[half]
        return remote(
            own.at[back_slot(step, way), pl.ds(start, size)], received.at[way, step - 1, pl.ds(start, size)],
            send, recv.at[step - 1, way, half], along[way],
        )

    bf = functools.partial(reduce_copy, pf, rf, F_PIECES, bf_send, bf_recv)
    bm = functools.partial(reduce_copy, pm, rm, M_PIECES, bm_send, bm_recv)

    def reduce_step(transfer, own, received, halves, step, chosen=None):
        count = len(halves)
        for way, half in chosen or back_parts_of(step, count):
            if step > 1 and (way, half) in back_parts_of(step - 1, count):
                transfer(step - 1, way, half).wait_recv()
                start, size = halves[half]
                slot = back_slot(step, way)
                own[slot, start:start + size, :] = (
                    own[slot, start:start + size, :].astype(F32)
                    + received[way, step - 2, start:start + size, :].astype(F32)
                ).astype(BF16)
            transfer(step, way, half).start()

    fresh, held = short_parts(2), far_parts(2)

    def one_way(parts, which):
        return [(way, half) for way, half in parts if way == which]


    def mix(slot):
        bn_all(slot).wait_recv()
        pm[slot] = jnp.dot(cn[...], rn[slot], preferred_element_type=F32).astype(BF16)

    def mix_down(index):
        mix(7 - index)

    def own_part(buffer):
        return jnp.dot(buffer[:, 0:HID], w2[7, 0:HID, :], preferred_element_type=F32)

    def other_part(buffer):
        return jnp.dot(buffer[:, HID:2 * HID], w2[7, HID:2 * HID, :], preferred_element_type=F32)

    first_near[...] = own_part(hn)
    first_far[...] = own_part(hf)
    for share in near_shares:
        share.wait_recv()
    send_back(7, (first_near[...] + other_part(hn)).astype(BF16))
    far_share.wait_recv()
    pf[7] = (first_far[...] + other_part(hf)).astype(BF16)
    reduce_step(bf, pf, rf, F_PIECES, 1)
    both(1, 3, far_out)
    reduce_step(bf, pf, rf, F_PIECES, 2, fresh)
    both(1, 3, near_out)
    logit_copy.wait()
    raised = jnp.exp(lg[...] + lg_other[...])
    probs = raised / jnp.sum(raised, axis=0, keepdims=True)
    chosen_first = jnp.sum(jnp.where(names == routing[0:1, :], probs, 0.0), axis=0, keepdims=True)
    chosen_second = jnp.sum(jnp.where(names == routing[1:2, :], probs, 0.0), axis=0, keepdims=True)
    packed = jnp.concatenate(
        [base[0:1, :], base[1:2, :], chosen_first, chosen_second, jnp.zeros((124, GROUP), F32)], axis=0
    )
    packed = jnp.transpose(packed)
    at_first, at_second = packed[:, 0:1].astype(jnp.int32), packed[:, 1:2].astype(jnp.int32)
    by_first, by_second = packed[:, 2:3], packed[:, 3:4]

    def weights(start, size):
        columns = lax.broadcasted_iota(jnp.int32, (GROUP, size), 1) + start
        return (
            jnp.where(columns == at_first, by_first, 0.0) + jnp.where(columns == at_second, by_second, 0.0)
        ).astype(BF16)

    cn[...] = weights(0, NR)
    cf[...] = weights(NR, FR)

    both(3, 5, far_out)
    reduce_step(bf, pf, rf, F_PIECES, 2, held)
    both(3, 4, near_out)
    reduce_step(bf, pf, rf, F_PIECES, 3, fresh)
    both(0, 1, mix_down)
    reduce_step(bm, pm, rm, M_PIECES, 1)
    both(5, 7, far_out)
    both(4, 5, near_out)
    both(1, 2, mix_down)
    reduce_step(bm, pm, rm, M_PIECES, 2, one_way(short_parts(4), 0))
    reduce_step(bf, pf, rf, F_PIECES, 3, held)
    both(5, 6, near_out)
    reduce_step(bf, pf, rf, F_PIECES, 4, fresh)
    both(2, 3, mix_down)
    reduce_step(bm, pm, rm, M_PIECES, 2, one_way(short_parts(4), 1))
    reduce_step(bm, pm, rm, M_PIECES, 2, far_parts(4))
    both(6, 7, near_out)
    both(7, 8, far_out)
    both(3, 4, mix_down)
    reduce_step(bf, pf, rf, F_PIECES, 4, held)
    both(7, 8, near_out)
    both(4, 5, mix_down)
    reduce_step(bm, pm, rm, M_PIECES, 3)

    both(5, 6, mix_down)
    for way, half in back_parts_of(4, 2):
        bf(4, way, half).wait_recv()
    fr[...] = (
        pf[0].astype(F32) + rf[0, 3].astype(F32) + rf[1, 3].astype(F32)
    ).astype(BF16)

    def far_back(p):
        block = pl.ds((p - NEAR) * CAP, CAP)
        return remote(fr.at[block], ra.at[block], ra_send, ra_recv, back[p])

    for p in FAR_ORDER:
        far_back(p).start()
    both(6, 7, mix_down)
    reduce_step(bm, pm, rm, M_PIECES, 4)
    both(7, 8, mix_down)
    remote(fr, ra, ra_send, ra_recv, sibling).wait_recv()
    far_term[...] = jnp.dot(cf[...], ra[...], preferred_element_type=F32) + pm[0].astype(F32)
    for way, half in back_parts_of(4, 4):
        bm(4, way, half).wait_recv()
    out[...] = (far_term[...] + rm[0, 3].astype(F32) + rm[1, 3].astype(F32)).astype(BF16)

    def sent(ref, semaphore):
        remote(ref, ref, semaphore, semaphore, sibling).wait_send()

    ring_blocks, most = pl.ds(0, Z - 1), pl.ds(0, NR - CAP)
    sent(tg.at[ring_blocks], f1_send)
    sent(far_send, a1_send)
    sent(near_send.at[:, most], f2_send)
    sent(xf.at[ring_blocks, 0], a2_send)
    sent(xn.at[:, 0], sn_send)
    sent(xf.at[:, 0], sf_send)
    sent(pf.at[ring_blocks], bf_send)
    sent(pm.at[ring_blocks], bm_send)
    sent(pn.at[:, most], bn_send)
    sent(fr, ra_send)
    w2_all.wait_send()
    for share in [*near_shares, far_share]:
        share.wait_send()


def layer(tokens, routing, gate_weight, expert_in, expert_out):
    vmem = pl.BlockSpec(memory_space=pltpu.VMEM)
    anywhere = pl.BlockSpec(memory_space=pl.ANY)
    dma = pltpu.SemaphoreType.DMA
    return pl.pallas_call(
        kernel,
        out_shape=pltpu.VMEM((GROUP, W), BF16),
        in_specs=[anywhere] * 5,
        out_specs=vmem,
        scratch_shapes=[
            pltpu.VMEM((Z, TB, W), BF16),
            pltpu.VMEM((EXPERTS * CAP, GROUP), BF16),
            pltpu.VMEM((Z, NR, W), BF16),
            pltpu.VMEM((FR, W), BF16),
            pltpu.VMEM((Z, 2, NR, W), BF16),
            pltpu.VMEM((Z, 2, FR, W), BF16),
            pltpu.VMEM((NR, HID), F32),
            pltpu.VMEM((FR, HID), F32),
            pltpu.VMEM((Z * 2 * W, HID), BF16),
            pltpu.VMEM((Z, 2 * HID, W), BF16),
            pltpu.VMEM((NR, 2 * HID), BF16),
            pltpu.VMEM((FR, 2 * HID), BF16),
            pltpu.VMEM((Z, FR, W), BF16),
            pltpu.VMEM((2, 4, FR, W), BF16),
            pltpu.VMEM((Z, NR, W), BF16),
            pltpu.VMEM((Z, NR, W), BF16),
            pltpu.VMEM((Z, GROUP, W), BF16),
            pltpu.VMEM((2, 4, GROUP, W), BF16),
            pltpu.VMEM((FR, W), BF16),
            pltpu.VMEM((FR, W), BF16),
            pltpu.VMEM((GROUP, NR), BF16),
            pltpu.VMEM((GROUP, FR), BF16),
            pltpu.VMEM((EXPERTS, GROUP), F32),
            pltpu.VMEM((EXPERTS, GROUP), F32),
            pltpu.VMEM((8, GROUP), F32),
            pltpu.VMEM((GROUP, W), F32),
            pltpu.VMEM((2, GROUP), jnp.int32),
            pltpu.VMEM((NR, W), F32),
            pltpu.VMEM((FR, W), F32),
            dma, dma, dma, dma, dma, dma, dma,
            dma, dma((4, 2, 2)), dma, dma, dma, dma((Z,)), dma, dma((4, 2, 2)),
            dma, dma((Z,)), dma, dma((Z,)), dma((3,)), dma((3,)), dma, dma,
            dma, dma((4, 2, 2)), dma, dma((Z,)), dma, dma((4, 2, 4)), dma, dma,
        ],
        compiler_params=pltpu.CompilerParams(collective_id=0, has_side_effects=True),
        name="experts",
    )(tokens, routing.T, gate_weight.T, expert_in, expert_out)


def solution(mesh):
    return jax.shard_map(
        layer,
        mesh=mesh,
        in_specs=(
            P("dp", "expert"),
            P("dp", None),
            P("expert", None),
            P("dp", None, "expert"),
            P("dp", "expert", None),
        ),
        out_specs=P("dp", "expert"),
        check_vma=False,
    )
```

```python
import functools

import jax
import jax.numpy as jnp
from jax import lax
from jax.experimental import pallas as pl
from jax.experimental.pallas import tpu as pltpu
from jax.sharding import PartitionSpec as P

MESH = pl.DeviceIdType.MESH
F32 = jnp.float32
BF16 = jnp.bfloat16

X, Y, Z = 4, 4, 8
GROUP, CAP, EXPERTS, W, HID = 256, 48, 16, 256, 512
SHIFTS = [(dx, dy) for dy in (-1, 0, 1) for dx in (-1, 0, 1)]
SHIFTS += [(2, 0), (0, 2), (2, -1), (2, 1), (2, 2), (-1, 2), (1, 2)]
NEAR, FAR, SELF = 11, 5, 4
NR, FR = NEAR * CAP, FAR * CAP
NEAR_ORDER = [0, 8, 9, 10, 2, 6, 1, 3, 7, 5]
FAR_ORDER = [13, 11, 14, 12, 15]
TB = GROUP + EXPERTS
T_PIECES = ((0, 128), (128, TB - 128))
F_PIECES = ((0, 3 * CAP), (3 * CAP, FR - 3 * CAP))
M_PIECES = ((0, 64), (64, 64), (128, 64), (192, 64))
N_PIECES = ((0, 6 * CAP), (6 * CAP, NR - 6 * CAP))


def far_parts(count):
    half = count // 2
    return [(way, i + half * way) for i in range(half) for way in (0, 1)]


def short_parts(count):
    half = count // 2
    return [(way, i + half * (1 - way)) for i in range(half) for way in (0, 1)]


def parts_of(step, count):
    return far_parts(count) if step == 4 else far_parts(count) + short_parts(count)


def back_parts_of(step, count):
    return far_parts(count) if step == 1 else short_parts(count) + far_parts(count)


def offset_of(slot):
    return 4 if slot == 7 else (slot // 2 if slot % 2 == 0 else -((slot + 1) // 2))


def gather_slots(step, way):
    source = 0 if step == 1 else 2 * step - 3 + way
    return source, (7 if step == 4 else 2 * step - 1 + way)


def back_slot(step, way):
    return 7 if step == 1 else 2 * (5 - step) - way


def kernel(
    tokens, picks, gate, w_in, w_out, out,
    tg, assign, near_send, far_send, xn, xf, acc_n, acc_f, w1, w2, hn, hf,
    pf, rf, pn, rn, pm, rm, fr, ra, cn, cf, lg, lg_other, base, far_term, routing, first_near, first_far,
    tok_sem, gate_sem, picks_sem, w1_sem, w2_sem, w2s_send, w2s_recv,
    f1_send, f1_recv, a1_send, a1_recv, f2_send, f2_recv, a2_send, a2_recv,
    sn_send, sn_recv, sf_send, sf_recv, h_send, h_recv, l_send, l_recv,
    bf_send, bf_recv, bn_send, bn_recv, bm_send, bm_recv, ra_send, ra_recv,
):
    dp = lax.axis_index("dp")
    ex = lax.axis_index("expert")
    gy, gx = lax.div(dp, X), lax.rem(dp, X)
    z, core = lax.div(ex, 2), lax.rem(ex, 2)

    def plane(dx, dy):
        return (lax.rem(gy + dy + Y, Y) * X + lax.rem(gx + dx + X, X), ex)

    def ring(offset):
        return lax.rem(z + offset + Z, Z)

    to = [plane(dx, dy) for dx, dy in SHIFTS]
    back = [plane(-dx, -dy) for dx, dy in SHIFTS]
    along = ((dp, ring(1) * 2 + 1 - core), (dp, ring(-1) * 2 + 1 - core))
    sibling = (dp, z * 2 + 1 - core)

    def remote(src, dst, send, recv, device):
        return pltpu.make_async_remote_copy(
            src_ref=src, dst_ref=dst, send_sem=send, recv_sem=recv,
            device_id=device, device_id_type=MESH,
        )

    barrier = pltpu.get_barrier_semaphore()
    for device in [to[p] for p in range(EXPERTS) if p != SELF] + [*along, sibling]:
        pl.semaphore_signal(barrier, inc=1, device_id=device, device_id_type=MESH)

    picks_copy = pltpu.make_async_copy(picks, routing, picks_sem)
    picks_copy.start()
    token_copy = pltpu.make_async_copy(tokens, tg.at[0, pl.ds(0, GROUP)], tok_sem)
    token_copy.start()
    gate_copy = pltpu.make_async_copy(gate, tg.at[0, pl.ds(GROUP, EXPERTS)], gate_sem)
    gate_copy.start()
    picks_copy.wait()

    def block_of(slot, side):
        offset = offset_of(slot)
        return ring(offset) * 2 + (core if (offset + side) % 2 == 0 else 1 - core)

    def w1_copy(slot, side):
        rows = block_of(slot, side) * W
        return pltpu.make_async_copy(
            w_in.at[0, pl.ds(pl.multiple_of(rows, W), W), :], w1.at[pl.ds((slot * 2 + side) * W, W)], w1_sem
        )

    def w2_columns(slot, side):
        columns = block_of(slot, side) * W
        return w_out.at[0, :, pl.ds(pl.multiple_of(columns, W), W)]

    def w2_copy(slot):
        return pltpu.make_async_copy(w2_columns(slot, 0), w2.at[slot, pl.ds(0, HID)], w2_sem)

    def w2_share(slot):
        return remote(
            w2_columns(slot, 1), w2.at[slot, pl.ds(HID, HID)], w2s_send, w2s_recv, sibling
        )

    def f1(step, way, half):
        source, target = gather_slots(step, way)
        start, size = T_PIECES[half]
        return remote(
            tg.at[source, pl.ds(start, size)], tg.at[target, pl.ds(start, size)],
            f1_send, f1_recv.at[step - 1, way, half], along[way],
        )

    def a1(p):
        block = pl.ds((p - NEAR) * CAP, CAP)
        return remote(far_send.at[block], xf.at[0, 0, block], a1_send, a1_recv, to[p])

    def f2(slot, p):
        block = pl.ds(p * CAP, CAP)
        return remote(
            near_send.at[slot, block], xn.at[slot, 0, block], f2_send, f2_recv.at[slot], to[p]
        )

    def f2_all(slot):
        block = pl.ds(0, NR - CAP)
        return remote(
            near_send.at[slot, block], xn.at[slot, 0, block], f2_send, f2_recv.at[slot], sibling
        )

    def a2(step, way, half):
        source, target = gather_slots(step, way)
        start, size = F_PIECES[half]
        return remote(
            xf.at[source, 0, pl.ds(start, size)], xf.at[target, 0, pl.ds(start, size)],
            a2_send, a2_recv.at[step - 1, way, half], along[way],
        )

    def share_near(slot):
        return remote(xn.at[slot, 0], xn.at[slot, 1], sn_send, sn_recv.at[slot], sibling)

    def share_far(slot):
        return remote(xf.at[slot, 0], xf.at[slot, 1], sf_send, sf_recv.at[slot], sibling)

    def send_near(slot):
        for p in NEAR_ORDER:
            f2(slot, p).start()

    def pass_on(transfer, step, chosen=None):
        for way, half in chosen or parts_of(step, 2):
            transfer(step, way, half).wait_recv()
            if step < 4 and (way, half) in parts_of(step + 1, 2):
                transfer(step + 1, way, half).start()

    names = lax.broadcasted_iota(jnp.int32, (EXPERTS, GROUP), 0)
    sx = (lax.rem(names, X) - gx + 1 + X) & 3
    sy = (lax.div(names, X) - gy + 1 + Y) & 3
    place = sy * 3 + sx
    for p in range(9, EXPERTS):
        dx, dy = SHIFTS[p]
        place = jnp.where((sx == dx + 1) & (sy == dy + 1), p, place)
    place = (place * CAP).astype(F32)
    first = (names == routing[0:1, :]).astype(F32)
    second = (names == routing[1:2, :]).astype(F32)
    earlier = lax.broadcasted_iota(jnp.int32, (GROUP, GROUP), 0)
    later = lax.broadcasted_iota(jnp.int32, (GROUP, GROUP), 1)
    upper = (earlier < later).astype(F32).astype(BF16)
    before_first = jnp.dot(first.astype(BF16), upper, preferred_element_type=F32)
    before_second = jnp.dot(second.astype(BF16), upper, preferred_element_type=F32)
    before_second = before_second + jnp.sum(first, axis=1, keepdims=True)
    row_first = jnp.sum(first * (place + before_first), axis=0, keepdims=True)
    row_second = jnp.sum(second * (place + before_second), axis=0, keepdims=True)
    rows = lax.broadcasted_iota(jnp.int32, (EXPERTS * CAP, GROUP), 0)
    hit = (rows == row_first.astype(jnp.int32)) | (rows == row_second.astype(jnp.int32))
    assign[...] = hit.astype(F32).astype(BF16)
    base[0:1, :] = row_first
    base[1:2, :] = row_second
    lg[...] = jnp.zeros_like(lg)

    token_copy.wait()
    gate_copy.wait()
    pl.semaphore_wait(barrier, 18)
    for way, half in parts_of(1, 2):
        f1(1, way, half).start()
    far_send[...] = jnp.dot(
        assign[NR:, :], tg[0, 0:GROUP, :], preferred_element_type=F32
    ).astype(BF16)

    def dispatch_near(slot):
        rows_of = jnp.dot(assign[0:NR, :], tg[slot, 0:GROUP, :], preferred_element_type=F32).astype(BF16)
        near_send[slot] = rows_of
        xn[slot, 0, SELF * CAP:(SELF + 1) * CAP, :] = rows_of[SELF * CAP:(SELF + 1) * CAP, :]
        lg[...] += lax.dot_general(
            tg[slot, GROUP:TB, :], tg[slot, 0:GROUP, :], (((1,), (1,)), ((), ())), preferred_element_type=F32
        )

    for p in FAR_ORDER:
        a1(p).start()
    dispatch_near(0)
    send_near(0)
    for slot in range(Z):
        for side in range(2):
            w1_copy(slot, side).start()
    for slot in range(Z):
        w2_copy(slot).start()

    acc_n[...] = jnp.zeros_like(acc_n)
    acc_f[...] = jnp.zeros_like(acc_f)

    none = lax.div(dp, X * Y)

    def both(lower, upper, work):
        lax.fori_loop(lower + none, upper + none, lambda slot, carry: (work(slot), carry)[1], 0)

    def near_part(slot):
        dispatch_near(slot)
        send_near(slot)

    def multiply(rows_of, total, slot, count):
        columns = [rows_of[slot + i, side] for i in range(count) for side in range(2)]
        depth = 2 * W * count
        start = pl.multiple_of(slot * 2 * W, 2 * W)
        total[...] += jnp.dot(
            jnp.concatenate(columns, axis=1), w1[pl.ds(start, depth), :], preferred_element_type=F32
        )

    def near_in(slot):
        f2_all(slot).wait_recv()
        share_near(slot).start()

    def near_multiply(slot, count=1):
        for i in range(count):
            share_near(slot + i).wait_recv()
        multiply(xn, acc_n, slot, count)

    def far_multiply(slot, count=1):
        for i in range(count):
            share_far(slot + i).wait_recv()
        multiply(xf, acc_f, slot, count)

    def w2_shares(lower, upper):
        for slot in range(lower, upper):
            w2_share(slot).start()

    for slot in range(4):
        w2_share(slot).start()
    pass_on(f1, 1)
    both(1, 3, near_part)
    for slot in range(4, Z):
        w2_share(slot).start()
    pl_all = pl.ds(0, FR)
    remote(far_send.at[pl_all], xf.at[0, 0, pl_all], a1_send, a1_recv, sibling).wait_recv()
    for way, half in far_parts(2):
        a2(1, way, half).start()
    share_far(0).start()
    pass_on(f1, 2)
    for way, half in short_parts(2):
        a2(1, way, half).start()
    both(3, 5, near_part)
    near_in(0)
    pltpu.make_async_copy(w_in.at[0], w1, w1_sem).wait()
    pass_on(a2, 1, far_parts(2))
    near_multiply(0, 1)
    far_multiply(0, 1)
    pass_on(f1, 3)
    both(5, 7, near_part)
    both(1, 3, near_in)
    pass_on(a2, 1, short_parts(2))
    share_far(1).start()
    share_far(2).start()
    pass_on(a2, 2, far_parts(2))
    pass_on(f1, 4)
    both(7, 8, near_part)

    logit_copy = remote(lg, lg_other, l_send, l_recv, sibling)
    logit_copy.start()
    both(3, 5, near_in)
    pass_on(a2, 2, short_parts(2))
    share_far(3).start()
    share_far(4).start()
    near_multiply(1, 2)
    far_multiply(1, 2)
    pass_on(a2, 3, far_parts(2))
    both(5, 7, near_in)
    near_multiply(3, 2)
    far_multiply(3, 2)
    pass_on(a2, 3, short_parts(2))
    share_far(5).start()
    share_far(6).start()
    near_in(7)
    near_multiply(5, 2)
    pass_on(a2, 4)
    share_far(7).start()
    far_multiply(5, 2)

    def share_hidden(buffer, start, size, which):
        rows = pl.ds(start, size)
        return remote(
            buffer.at[rows, pl.ds(0, HID)], buffer.at[rows, pl.ds(HID, HID)],
            h_send.at[which], h_recv.at[which], sibling,
        )

    near_shares = [share_hidden(hn, start, size, which) for which, (start, size) in enumerate(N_PIECES)]
    far_share = share_hidden(hf, 0, FR, 2)
    share_near(7).wait_recv()
    for share, (start, size) in zip(near_shares, N_PIECES):
        stop = start + size
        total = acc_n[start:stop, :] + jnp.dot(
            jnp.concatenate([xn[7, 0, start:stop, :], xn[7, 1, start:stop, :]], axis=1),
            w1[14 * W:16 * W, :], preferred_element_type=F32,
        )
        hn[start:stop, 0:HID] = jax.nn.gelu(total, approximate=True).astype(BF16)
        share.start()
    far_multiply(7, 1)
    hf[:, 0:HID] = jax.nn.gelu(acc_f[...], approximate=True).astype(BF16)
    far_share.start()
    own_half, other_half = w2.at[:, pl.ds(0, HID)], w2.at[:, pl.ds(HID, HID)]
    pltpu.make_async_copy(own_half, own_half, w2_sem).wait()
    w2_all = remote(own_half, other_half, w2s_send, w2s_recv, sibling)
    w2_all.wait_recv()

    def bn(slot, p):
        block = pl.ds(p * CAP, CAP)
        return remote(
            pn.at[slot, block], rn.at[slot, block], bn_send, bn_recv.at[slot], back[p]
        )

    def bn_all(slot):
        block = pl.ds(0, NR - CAP)
        return remote(
            pn.at[slot, block], rn.at[slot, block], bn_send, bn_recv.at[slot], sibling
        )

    def second(buffer, slot):
        return jnp.dot(buffer[...], w2[slot], preferred_element_type=F32).astype(BF16)

    def near_out(index):
        slot = 7 - index
        send_back(slot, second(hn, slot))

    def send_back(slot, terms):
        pn[slot] = terms
        rn[slot, SELF * CAP:(SELF + 1) * CAP, :] = terms[SELF * CAP:(SELF + 1) * CAP, :]
        for p in NEAR_ORDER:
            bn(slot, p).start()

    def far_out(index):
        slot = 7 - index
        pf[slot] = second(hf, slot)

    def reduce_copy(own, received, halves, send, recv, step, way, half):
        start, size = halves[half]
        return remote(
            own.at[back_slot(step, way), pl.ds(start, size)], received.at[way, step - 1, pl.ds(start, size)],
            send, recv.at[step - 1, way, half], along[way],
        )

    bf = functools.partial(reduce_copy, pf, rf, F_PIECES, bf_send, bf_recv)
    bm = functools.partial(reduce_copy, pm, rm, M_PIECES, bm_send, bm_recv)

    def reduce_step(transfer, own, received, halves, step, chosen=None):
        count = len(halves)
        for way, half in chosen or back_parts_of(step, count):
            if step > 1 and (way, half) in back_parts_of(step - 1, count):
                transfer(step - 1, way, half).wait_recv()
                start, size = halves[half]
                slot = back_slot(step, way)
                own[slot, start:start + size, :] = (
                    own[slot, start:start + size, :].astype(F32)
                    + received[way, step - 2, start:start + size, :].astype(F32)
                ).astype(BF16)
            transfer(step, way, half).start()

    fresh, held = short_parts(2), far_parts(2)

    def one_way(parts, which):
        return [(way, half) for way, half in parts if way == which]


    def mix(slot):
        bn_all(slot).wait_recv()
        pm[slot] = jnp.dot(cn[...], rn[slot], preferred_element_type=F32).astype(BF16)

    def mix_down(index):
        mix(7 - index)

    def own_part(buffer):
        return jnp.dot(buffer[:, 0:HID], w2[7, 0:HID, :], preferred_element_type=F32)

    def other_part(buffer):
        return jnp.dot(buffer[:, HID:2 * HID], w2[7, HID:2 * HID, :], preferred_element_type=F32)

    first_near[...] = own_part(hn)
    first_far[...] = own_part(hf)
    for share in near_shares:
        share.wait_recv()
    send_back(7, (first_near[...] + other_part(hn)).astype(BF16))
    far_share.wait_recv()
    pf[7] = (first_far[...] + other_part(hf)).astype(BF16)
    reduce_step(bf, pf, rf, F_PIECES, 1)
    both(1, 3, far_out)
    reduce_step(bf, pf, rf, F_PIECES, 2, fresh)
    both(1, 3, near_out)
    logit_copy.wait()
    raised = jnp.exp(lg[...] + lg_other[...])
    probs = raised / jnp.sum(raised, axis=0, keepdims=True)
    chosen_first = jnp.sum(jnp.where(names == routing[0:1, :], probs, 0.0), axis=0, keepdims=True)
    chosen_second = jnp.sum(jnp.where(names == routing[1:2, :], probs, 0.0), axis=0, keepdims=True)
    packed = jnp.concatenate(
        [base[0:1, :], base[1:2, :], chosen_first, chosen_second, jnp.zeros((124, GROUP), F32)], axis=0
    )
    packed = jnp.transpose(packed)
    at_first, at_second = packed[:, 0:1].astype(jnp.int32), packed[:, 1:2].astype(jnp.int32)
    by_first, by_second = packed[:, 2:3], packed[:, 3:4]

    def weights(start, size):
        columns = lax.broadcasted_iota(jnp.int32, (GROUP, size), 1) + start
        return (
            jnp.where(columns == at_first, by_first, 0.0) + jnp.where(columns == at_second, by_second, 0.0)
        ).astype(BF16)

    cn[...] = weights(0, NR)
    cf[...] = weights(NR, FR)

    both(3, 5, far_out)
    reduce_step(bf, pf, rf, F_PIECES, 2, held)
    both(3, 4, near_out)
    reduce_step(bf, pf, rf, F_PIECES, 3, fresh)
    both(0, 1, mix_down)
    reduce_step(bm, pm, rm, M_PIECES, 1)
    both(5, 7, far_out)
    both(4, 5, near_out)
    both(1, 2, mix_down)
    reduce_step(bm, pm, rm, M_PIECES, 2, one_way(short_parts(4), 0))
    reduce_step(bf, pf, rf, F_PIECES, 3, held)
    both(5, 6, near_out)
    both(2, 3, mix_down)
    reduce_step(bm, pm, rm, M_PIECES, 2, one_way(short_parts(4), 1))
    reduce_step(bm, pm, rm, M_PIECES, 2, far_parts(4))
    reduce_step(bf, pf, rf, F_PIECES, 4, fresh)
    both(6, 7, near_out)
    both(7, 8, far_out)
    both(3, 4, mix_down)
    reduce_step(bf, pf, rf, F_PIECES, 4, held)
    both(7, 8, near_out)
    both(4, 5, mix_down)
    reduce_step(bm, pm, rm, M_PIECES, 3)

    both(5, 6, mix_down)
    for way, half in back_parts_of(4, 2):
        bf(4, way, half).wait_recv()
    fr[...] = (
        pf[0].astype(F32) + rf[0, 3].astype(F32) + rf[1, 3].astype(F32)
    ).astype(BF16)

    def far_back(p):
        block = pl.ds((p - NEAR) * CAP, CAP)
        return remote(fr.at[block], ra.at[block], ra_send, ra_recv, back[p])

    for p in FAR_ORDER:
        far_back(p).start()
    both(6, 7, mix_down)
    reduce_step(bm, pm, rm, M_PIECES, 4)
    both(7, 8, mix_down)
    remote(fr, ra, ra_send, ra_recv, sibling).wait_recv()
    far_term[...] = jnp.dot(cf[...], ra[...], preferred_element_type=F32) + pm[0].astype(F32)
    for way, half in back_parts_of(4, 4):
        bm(4, way, half).wait_recv()
    out[...] = (far_term[...] + rm[0, 3].astype(F32) + rm[1, 3].astype(F32)).astype(BF16)

    def sent(ref, semaphore):
        remote(ref, ref, semaphore, semaphore, sibling).wait_send()

    ring_blocks, most = pl.ds(0, Z - 1), pl.ds(0, NR - CAP)
    sent(tg.at[ring_blocks], f1_send)
    sent(far_send, a1_send)
    sent(near_send.at[:, most], f2_send)
    sent(xf.at[ring_blocks, 0], a2_send)
    sent(xn.at[:, 0], sn_send)
    sent(xf.at[:, 0], sf_send)
    sent(pf.at[ring_blocks], bf_send)
    sent(pm.at[ring_blocks], bm_send)
    sent(pn.at[:, most], bn_send)
    sent(fr, ra_send)
    w2_all.wait_send()
    for share in [*near_shares, far_share]:
        share.wait_send()


def layer(tokens, routing, gate_weight, expert_in, expert_out):
    vmem = pl.BlockSpec(memory_space=pltpu.VMEM)
    anywhere = pl.BlockSpec(memory_space=pl.ANY)
    dma = pltpu.SemaphoreType.DMA
    return pl.pallas_call(
        kernel,
        out_shape=pltpu.VMEM((GROUP, W), BF16),
        in_specs=[anywhere] * 5,
        out_specs=vmem,
        scratch_shapes=[
            pltpu.VMEM((Z, TB, W), BF16),
            pltpu.VMEM((EXPERTS * CAP, GROUP), BF16),
            pltpu.VMEM((Z, NR, W), BF16),
            pltpu.VMEM((FR, W), BF16),
            pltpu.VMEM((Z, 2, NR, W), BF16),
            pltpu.VMEM((Z, 2, FR, W), BF16),
            pltpu.VMEM((NR, HID), F32),
            pltpu.VMEM((FR, HID), F32),
            pltpu.VMEM((Z * 2 * W, HID), BF16),
            pltpu.VMEM((Z, 2 * HID, W), BF16),
            pltpu.VMEM((NR, 2 * HID), BF16),
            pltpu.VMEM((FR, 2 * HID), BF16),
            pltpu.VMEM((Z, FR, W), BF16),
            pltpu.VMEM((2, 4, FR, W), BF16),
            pltpu.VMEM((Z, NR, W), BF16),
            pltpu.VMEM((Z, NR, W), BF16),
            pltpu.VMEM((Z, GROUP, W), BF16),
            pltpu.VMEM((2, 4, GROUP, W), BF16),
            pltpu.VMEM((FR, W), BF16),
            pltpu.VMEM((FR, W), BF16),
            pltpu.VMEM((GROUP, NR), BF16),
            pltpu.VMEM((GROUP, FR), BF16),
            pltpu.VMEM((EXPERTS, GROUP), F32),
            pltpu.VMEM((EXPERTS, GROUP), F32),
            pltpu.VMEM((8, GROUP), F32),
            pltpu.VMEM((GROUP, W), F32),
            pltpu.VMEM((2, GROUP), jnp.int32),
            pltpu.VMEM((NR, W), F32),
            pltpu.VMEM((FR, W), F32),
            dma, dma, dma, dma, dma, dma, dma,
            dma, dma((4, 2, 2)), dma, dma, dma, dma((Z,)), dma, dma((4, 2, 2)),
            dma, dma((Z,)), dma, dma((Z,)), dma((3,)), dma((3,)), dma, dma,
            dma, dma((4, 2, 2)), dma, dma((Z,)), dma, dma((4, 2, 4)), dma, dma,
        ],
        compiler_params=pltpu.CompilerParams(collective_id=0, has_side_effects=True),
        name="experts",
    )(tokens, routing.T, gate_weight.T, expert_in, expert_out)


def solution(mesh):
    return jax.shard_map(
        layer,
        mesh=mesh,
        in_specs=(
            P("dp", "expert"),
            P("dp", None),
            P("expert", None),
            P("dp", None, "expert"),
            P("dp", "expert", None),
        ),
        out_specs=P("dp", "expert"),
        check_vma=False,
    )
```
